32 devices in a mesh: group: 2 (over core), gx: 4 (over y, x), gy: 4 (over z).
Axes of the slice: x: 2, y: 2, z: 4, core: 2. Of those that a mesh axis runs over, the one named last changes fastest.
Arguments:
- forcing: float32 [2, 80, 32, 1024], P('group', None, 'gx', 'gy'), may hold values from -24 to 24
- conduct: bfloat16 [2, 80, 32, 1024], P('group', None, 'gx', 'gy'), may hold values from 0.25 to 4
- diag_add: bfloat16 [2, 80, 32, 1024], P('group', None, 'gx', 'gy'), may hold values from 0.049804688 to 0.5
- ice_mask: int32 [32, 1024], P('gx', 'gy'), may hold values 0 or 1
- grounded: int32 [32, 1024], P('gx', 'gy'), may hold values 0 or 1
Outputs:
- solution: float32 [2, 80, 32, 1024], P('group', None, 'gx', 'gy')
- residual: float32 [2, 80, 32, 1024], P('group', None, 'gx', 'gy')
The draws below stay inside these ranges and needn't reach their ends.
All inputs are finite; a program needn't handle non-finite values. No bound on the sum of `ice_mask` or of `grounded` on one device may be relied on, other than what follows from the above.
Results may differ from the reference program's by a relative error of at most 0.0003.
Values sent between devices are 32-bit elements; how exact they have to be, the bound alone decides.
A program may use at most 64 MiB of HBM per device.

```python
import math
import jax
import jax.numpy as jnp
from jax import lax

LAYERS = 80
ITERS = 6
NX = 32
NY = 1024


def place_ends(result, own_key, low, high):
    longest = result.shape.index(max(result.shape))
    spots = []
    for shift in (0, 1):
        where = [jax.random.randint(jax.random.fold_in(own_key, axis), (), 0, length) for axis, length in enumerate(result.shape)]
        where[longest] = (where[longest] + shift) % result.shape[longest]
        spots.append(tuple(where))
    return result.at[spots[0]].set(low).at[spots[1]].set(high)


def steps_of(key, dims, cuts, low, largest):
    def one(dim, parts):
        steps = jax.random.uniform(jax.random.fold_in(jax.random.fold_in(key, 6), dim), (parts,), jnp.float32, low / len(cuts), largest / len(cuts))
        return jnp.repeat(jnp.exp(steps), dims[dim] // parts).reshape((-1,) + (1,) * (len(dims) - dim - 1))

    loudness = one(*cuts[0])
    for cut in cuts[1:]:
        loudness = loudness * one(*cut)
    return loudness


def noise(stream_key, shape, scale, most, pieces=(), held_as=jnp.bfloat16):
    entries = jax.random.normal(stream_key, shape, jnp.float32) * scale
    if len(pieces) > 0:
        entries = steps_of(stream_key, shape, pieces, -0.22, 0.18) * entries
    return jnp.clip(entries, min=-most, max=most).astype(held_as)


def setup_inputs(seed: int = 0) -> dict:
    streams_of = jax.random.split(jax.random.key(seed), 6)
    forcing = noise(streams_of[0], (2, LAYERS, NX, NY), 4.0, 24.0, ((0, 2), (2, 4), (3, 4)), jnp.float32)
    conduct = jnp.clip(jnp.exp(math.log(4.0) - 2.7725887 * jax.random.uniform(streams_of[1], (2, LAYERS, NX, NY), jnp.float32) ** steps_of(streams_of[1], (2, LAYERS, NX, NY), ((0, 2), (2, 4), (3, 4)), -0.2, 0.2)), 0.25, 4.0).astype(jnp.bfloat16)
    diag_add = jnp.clip(jnp.exp(math.log(0.5) - 2.306499 * jax.random.uniform(streams_of[2], (2, LAYERS, NX, NY), jnp.float32) ** steps_of(streams_of[2], (2, LAYERS, NX, NY), ((0, 2), (2, 4), (3, 4)), -0.2, 0.2)), 0.049804688, 0.5).astype(jnp.bfloat16)
    ice_mask = place_ends((jax.random.randint(streams_of[3], (NX, NY), 0, 8) < 7).astype(jnp.int32), jax.random.fold_in(streams_of[3], 1), 0, 1)
    grounded = place_ends((jax.random.randint(streams_of[4], (NX, NY), 0, 8) < 3).astype(jnp.int32), jax.random.fold_in(streams_of[4], 1), 0, 1)
    return dict(forcing=forcing, conduct=conduct, diag_add=diag_add, ice_mask=ice_mask, grounded=grounded)


far_weight = 0.25
cross_weight = 0.5
vertical_weight = 4.0
friction_gain = 8.0
NEIGHBOURS = ((1, 0, 1.0), (-1, 0, 1.0), (0, 1, 1.0), (0, -1, 1.0), (2, 0, far_weight), (-2, 0, far_weight), (0, 2, far_weight), (0, -2, far_weight), (1, 1, cross_weight), (1, -1, cross_weight), (-1, 1, cross_weight), (-1, -1, cross_weight))

def beside_sum(padded, extent_x, extent_y):
    summed = jnp.zeros((padded.shape[0], extent_x, extent_y), jnp.float32)
    for shift_x, shift_y, weight in NEIGHBOURS:
        summed = summed + weight * padded[:, 2 + shift_x:2 + shift_x + extent_x, 2 + shift_y:2 + shift_y + extent_y]
    return summed

def vertical_sum(values):
    zeroes = jnp.zeros_like(values[:1])
    return jnp.concatenate([values[1:], zeroes], 0) + jnp.concatenate([zeroes, values[:-1]], 0)

def spread(values):
    padded = jnp.pad(values, ((0, 0), (2, 2), (2, 2)))
    return beside_sum(padded, values.shape[1], values.shape[2]) + vertical_weight * vertical_sum(values)

def group_setup(group_id, forcing, conduct, diag_add, ice_mask, grounded):
    ice_cells = ice_mask.astype(jnp.float32)
    ground_cells = grounded.astype(jnp.float32)
    if group_id == 0:
        active = ice_cells
    else:
        active = ice_cells * (1.0 - ground_cells)
    layers = forcing.shape[1]
    coupling = jnp.sqrt(conduct[group_id].astype(jnp.float32)) * active
    base_diag = diag_add[group_id].astype(jnp.float32)
    if group_id == 0:
        base_diag = base_diag.at[0].add(friction_gain * ground_cells * ice_cells)
    diagonal = base_diag + coupling * spread(coupling)
    edge_layer = 0 if group_id == 0 else layers - 1
    shared_value = active * lax.optimization_barrier(jnp.mean(forcing[group_id], axis=0))
    shared_weight = coupling[edge_layer]
    return (active, coupling, diagonal, edge_layer, shared_value, shared_weight)

def solve(source, coupling, diagonal):
    inverse = 1.0 / diagonal
    solution = jnp.zeros_like(source)
    residual = source
    precond = inverse * residual
    direction = precond
    norm_now = jnp.sum(residual * precond)
    for iteration in range(ITERS):
        applied = diagonal * direction - coupling * spread(coupling * direction)
        step_size = norm_now / jnp.sum(direction * applied)
        solution = solution + step_size * direction
        residual = residual - step_size * applied
        if iteration + 1 < ITERS:
            precond = inverse * residual
            norm_next = jnp.sum(residual * precond)
            direction = precond + norm_next / norm_now * direction
            norm_now = norm_next
    return (solution, residual)

def reference(forcing, conduct, diag_add, ice_mask, grounded):
    setups = [group_setup(group_id, forcing, conduct, diag_add, ice_mask, grounded) for group_id in (0, 1)]
    solutions = []
    residuals = []
    for group_id in (0, 1):
        active, coupling, diagonal, edge_layer, shared_value, shared_weight = setups[group_id]
        partner = setups[1 - group_id]
        source = active * forcing[group_id]
        source = source.at[edge_layer].add(active * partner[5] * partner[4])
        solution, residual = solve(source, coupling, diagonal)
        solutions.append(solution)
        residuals.append(residual)
    return (jnp.stack(solutions), jnp.stack(residuals))
```

```python
import functools

import jax
import jax.numpy as jnp
from jax import lax
from jax.experimental import pallas as pl
from jax.experimental.pallas import tpu as pltpu
from jax.sharding import PartitionSpec as P

ITERS = 6
far_weight = 0.25
cross_weight = 0.5
vertical_weight = 4.0
friction_gain = 8.0
SUB = 8
LANES = 128
CHUNK_TILES = (1,)


def coefficients(moments):
    def gram(j, k):
        return 0.5 * (moments[j + k] + moments[abs(j - k)])

    table = {(j, k): gram(j, k) for j in range(ITERS + 1) for k in range(j, ITERS + 1)}

    def form(a, b):
        terms = []
        for j in range(len(a)):
            row = None
            for k in range(len(b)):
                term = table[min(j, k), max(j, k)] * b[k]
                row = term if row is None else row + term
            terms.append(a[j] * row)
        return functools.reduce(lambda s, t: s + t, terms)

    def shift(e):
        out = [jnp.zeros_like(e[0]) for _ in range(len(e) + 1)]
        for k, value in enumerate(e):
            if k == 0:
                out[1] = out[1] + value
            else:
                out[k + 1] = out[k + 1] + 0.5 * value
                out[k - 1] = out[k - 1] + 0.5 * value
        return out

    left = [jnp.ones_like(moments[0])]
    direction = list(left)
    iterate = []
    norm_now = form(left, left)
    for iteration in range(ITERS):
        moved = shift(direction)
        applied = [
            (direction[k] - moved[k]) if k < len(direction) else -moved[k]
            for k in range(len(moved))
        ]
        step = norm_now / form(direction, applied)
        iterate = [
            (iterate[k] if k < len(iterate) else 0.0) + step * direction[k]
            for k in range(len(direction))
        ]
        left = [
            (left[k] - step * applied[k]) if k < len(left) else -step * applied[k]
            for k in range(len(applied))
        ]
        if iteration + 1 < ITERS:
            norm_next = form(left, left)
            ratio = norm_next / norm_now
            direction = [
                left[k] + (ratio * direction[k] if k < len(direction) else 0.0)
                for k in range(len(left))
            ]
            norm_now = norm_next
    return iterate, left


def kernel(
    sizes,
    force,
    conduct,
    extra,
    ice,
    grounded,
    out_x,
    out_r,
    field,
    pack,
    rim_right,
    rim_left,
    corner,
    cornered,
    held,
    basis,
    coupling,
    scaled,
    diagonal,
    share,
    shared,
    partial,
    sum_x,
    sum_y,
    send_sem,
    recv_sem,
    share_sem,
    detour_sem,
    sx_send,
    sx_recv,
    sy_send,
    sy_recv,
):
    nx, ny = sizes
    rows, layers, width = force.shape
    tiles = layers // SUB
    chunks = corner.shape[1]
    per = tiles // chunks
    deep = per * SUB
    gg, gx, gy = lax.axis_index("group"), lax.axis_index("gx"), lax.axis_index("gy")
    is_ice = gg == 0

    def there(dx, dy):
        ok = None
        for d, g, n in ((dx, gx, nx), (dy, gy, ny)):
            if d != 0:
                one = (g + d >= 0) & (g + d < n)
                ok = one if ok is None else ok & one
        return ok

    def at(dx, dy):
        return (gg, gx + dx, gy + dy)

    two = 2 * rows
    sides = ((-1, 0), (1, 0), (0, -1), (0, 1), (-1, -1), (1, -1), (-1, 1), (1, 1))

    def copy_of(i, p, c, span=2):
        dx, dy = sides[i]
        inner = pl.ds(pl.multiple_of(c * deep + SUB, SUB), deep)
        flat = pl.ds(pl.multiple_of(c * deep, SUB), deep)
        if i == 0:
            source = field.at[p, 2 : 2 + span, inner]
            target = field.at[p, rows + 2 : rows + 2 + span, inner]
        elif i == 1:
            source = field.at[p, rows : rows + span, inner]
            target = field.at[p, 0:span, inner]
        elif i == 2:
            source, target = pack.at[p, flat], rim_right.at[p, flat]
        elif i == 3:
            source, target = pack.at[p, flat], rim_left.at[p, flat]
        else:
            source, target = corner.at[p, c], cornered.at[p, c, i - 4]
        return pltpu.make_async_remote_copy(
            src_ref=source,
            dst_ref=target,
            send_sem=send_sem.at[p, c, i],
            recv_sem=recv_sem.at[p, c, i],
            device_id=at(dx, dy),
            device_id_type=pl.DeviceIdType.MESH,
        )

    detours = ((1, 3, 2, rows, 0), (2, 0, 1, 2, rows + 2)) if nx == 4 else ()
    relayed = gg == 1
    lag = min(3, chunks - 1)

    def each(toward, act):
        for i, (dx, dy) in enumerate(sides):
            ok = there(toward * dx, toward * dy)
            if i < 2 and detours:
                split = gx == ((2 - i) if toward > 0 else (1 + i))

                ok = ok & jnp.logical_not(split & relayed)

            @pl.when(ok)
            def _():
                act(i, 2)

    def away(path, p, c, slot):
        origin, relay, _, row, _ = path
        return pltpu.make_async_remote_copy(
            src_ref=field.at[p, row : row + 2, pl.ds(pl.multiple_of(c * deep + SUB, SUB), deep)],
            dst_ref=held.at[slot, :, pl.ds(pl.multiple_of(c * deep, SUB), deep)],
            send_sem=detour_sem.at[0, p, c],
            recv_sem=detour_sem.at[1, p, c],
            device_id=(gg, relay, gy),
            device_id_type=pl.DeviceIdType.MESH,
        )

    def onward(path, p, c, slot):
        _, _, end, _, row = path
        return pltpu.make_async_remote_copy(
            src_ref=held.at[slot, :, pl.ds(pl.multiple_of(c * deep, SUB), deep)],
            dst_ref=field.at[p, row : row + 2, pl.ds(pl.multiple_of(c * deep + SUB, SUB), deep)],
            send_sem=detour_sem.at[2, p, c],
            recv_sem=detour_sem.at[3, p, c],
            device_id=(gg, end, gy),
            device_id_type=pl.DeviceIdType.MESH,
        )

    def forward(message):
        slot = message // chunks
        c = message % chunks
        p = slot % 2
        for path in detours:
            @pl.when((gx == path[1]) & relayed)
            def _():
                @pl.when(slot >= 2)
                def _():
                    onward(path, p, c, slot).wait_send()

                away(path, p, c, slot).wait_recv()
                onward(path, p, c, slot).start()

    def start(p, c, slot):
        for path in detours:
            @pl.when((gx == path[0]) & relayed)
            def _():
                away(path, p, c, slot).start()
        each(1, lambda i, span: copy_of(i, p, c, span).start())

    def finish_recv(p, c):
        for path in detours:
            @pl.when((gx == path[2]) & relayed)
            def _():
                onward(path, p, c, 0).wait_recv()
        each(-1, lambda i, span: copy_of(i, p, c, span).wait_recv())

    def finish_send(p, c):
        for path in detours:
            @pl.when((gx == path[0]) & relayed)
            def _():
                away(path, p, c, 0).wait_send()
        each(1, lambda i, span: copy_of(i, p, c, span).wait_send())

    for p in range(2):
        for r, d in ((0, -1), (rows + 2, 1)):
            @pl.when(jnp.logical_not(there(d, 0)))
            def _():
                field[p, r : r + 2] = jnp.zeros((2, layers + 2 * SUB, width), jnp.float32)
        for r in range(2, rows + 2):
            for s in (0, SUB + layers):
                field[p, r, s : s + SUB] = jnp.zeros((SUB, width), jnp.float32)
        for ref, d in ((rim_left, -1), (rim_right, 1)):
            @pl.when(jnp.logical_not(there(0, d)))
            def _():
                ref[p] = jnp.zeros(ref.shape[1:], jnp.float32)
        for i in range(4):
            @pl.when(jnp.logical_not(there(-sides[4 + i][0], -sides[4 + i][1])))
            def _():
                for c in range(chunks):
                    cornered[p, c, i] = jnp.zeros((1, LANES), jnp.float32)

    barrier = pltpu.get_barrier_semaphore()

    def greet(device):
        pl.semaphore_signal(
            barrier, inc=1, device_id=device, device_id_type=pl.DeviceIdType.MESH
        )

    greet((1 - gg, gx, gy))
    for o in range(1, nx):
        greet((gg, lax.rem(gx + o, nx), gy))
    for o in range(1, ny):
        greet((gg, gx, lax.rem(gy + o, ny)))
    met = jnp.int32(1 + nx - 1 + ny - 1)
    for dx, dy in sides[4:]:
        @pl.when(there(dx, dy))
        def _():
            greet(at(dx, dy))
        met = met + jnp.where(there(dx, dy), 1, 0).astype(jnp.int32)

    lane = lax.broadcasted_iota(jnp.int32, (SUB, LANES), 1)
    sub = lax.broadcasted_iota(jnp.int32, (SUB, width), 0)

    tile_row = lax.broadcasted_iota(jnp.int32, (SUB, LANES), 0)

    def spot(i, t):
        return lane == (i * per + t) * SUB + tile_row

    def pack_row(x, value, tile, t, corners):
        first, last = value[:, :LANES], value[:, width - LANES :]
        low = first if x == 0 else pltpu.roll(first, 2 * x, 1)
        high = pltpu.roll(last, (two + 2 * x - LANES + 2) % LANES, 1)
        tile = jnp.where((lane >= 2 * x) & (lane < 2 * x + 2), low, tile)
        tile = jnp.where((lane >= two + 2 * x) & (lane < two + 2 * x + 2), high, tile)
        for i, (at_x, y) in enumerate(
            ((0, 0), (rows - 1, 0), (0, width - 1), (rows - 1, width - 1))
        ):
            if x == at_x:
                column = jnp.broadcast_to(value[:, y : y + 1], (SUB, LANES))
                corners = jnp.where(spot(i, t), column, corners)
        return tile, corners

    def put_corner(p, c, corners):
        corner[p, c] = jnp.sum(corners, axis=0, keepdims=True)

    ice_cells = ice[...].astype(jnp.float32)
    ground_cells = grounded[...].astype(jnp.float32)
    ocean = jnp.where(is_ice, 0.0, 1.0).astype(jnp.float32)
    active = ice_cells * (1.0 - ocean * ground_cells)
    friction = (1.0 - ocean) * friction_gain * ground_cells * ice_cells

    def wide(array, x):
        return jnp.broadcast_to(array[x : x + 1, :], (SUB, width))

    blank = jnp.zeros((SUB, LANES), jnp.float32)
    zero = jnp.zeros((SUB, width), jnp.float32)

    def first_pass(c, sums):
        @pl.when(c >= lag)
        def _():
            forward(c - lag)

        corners = blank
        for t in range(per):
            j = c * per + t
            ls = pl.ds(pl.multiple_of(j * SUB, SUB), SUB)
            tile, after = blank, []
            for x in range(rows):
                value = jnp.sqrt(conduct[x, ls, :]) * wide(active, x)
                coupling[x, ls, :] = value
                field[0, x + 2, pl.ds(pl.multiple_of(j * SUB + SUB, SUB), SUB), :] = value
                tile, corners = pack_row(x, value, tile, t, corners)
                after.append(sums[x] + force[x, ls, :])
            sums = tuple(after)
            pack[0, ls, :] = tile
        put_corner(0, c, corners)
        start(0, c, 0)
        return sums

    pl.semaphore_wait(barrier, met)
    sums = lax.fori_loop(0, chunks, first_pass, (zero,) * rows)
    for x in range(rows):
        mean = jnp.sum(sums[x], axis=0, keepdims=True) * (1.0 / layers)
        share[0, x : x + 1, :] = active[x : x + 1, :] * mean
        share[1, x : x + 1, :] = jnp.where(
            is_ice, coupling[x, 0:1, :], coupling[x, layers - 1 : layers, :]
        )

    to_partner = pltpu.make_async_remote_copy(
        src_ref=share,
        dst_ref=shared,
        send_sem=share_sem.at[0],
        recv_sem=share_sem.at[1],
        device_id=(1 - gg, gx, gy),
        device_id_type=pl.DeviceIdType.MESH,
    )
    to_partner.start()

    def spread_block(p, c, t):
        j = c * per + t
        here = pl.ds(pl.multiple_of(j * SUB + SUB, SUB), SUB)
        below = pl.ds(pl.multiple_of(j * SUB, SUB), SUB)
        above = pl.ds(pl.multiple_of(j * SUB + 2 * SUB, SUB), SUB)
        from_right, from_left = rim_right[p, below, :], rim_left[p, below, :]

        def column(i):
            row = jnp.broadcast_to(cornered[p, c, i], (SUB, LANES))
            return jnp.sum(jnp.where(spot(i, t), row, 0.0), axis=1, keepdims=True)

        def rim(x):
            right = from_right if x == 0 else pltpu.roll(from_right, LANES - 2 * x, 1)
            left = pltpu.roll(from_left, (LANES - 2 - two - 2 * x) % LANES, 1)
            return jnp.where(lane < LANES // 2, right, left)

        def line(x):
            if x == 0:
                edge = jnp.where(lane < LANES // 2, column(1), column(3))
            elif x == rows + 1:
                edge = jnp.where(lane < LANES // 2, column(0), column(2))
            else:
                edge = rim(x - 1)
            value = field[p, x + 1, here, :]
            return [value[:, l : l + LANES] for l in range(0, width, LANES)] + [edge]

        def shifted(tiles_in, by):
            count = len(tiles_in) - 1
            out = []
            for i in range(count):
                before, own, after = tiles_in[i - 1], tiles_in[i], tiles_in[i + 1]
                up = pltpu.roll(jnp.where(lane >= LANES - by, before, own), by, 1)
                down = pltpu.roll(jnp.where(lane < by, after, own), LANES - by, 1)
                out.append(up + down)
            return jnp.concatenate(out, axis=1)

        e = [line(0), line(1)]
        for x in range(rows):
            e.append(line(x + 2))
            beside = [a + b for a, b in zip(e[x], e[x + 2])]
            h = [a + cross_weight * b for a, b in zip(e[x + 1], beside)]
            mine = field[p, x + 2, here, :]
            up = pltpu.roll(jnp.where(sub == 0, field[p, x + 2, above, :], mine), SUB - 1, 0)
            down = pltpu.roll(jnp.where(sub == SUB - 1, field[p, x + 2, below, :], mine), 1, 0)
            yield (
                shifted(h, 1)
                + jnp.concatenate(beside[:-1], axis=1)
                + far_weight
                * (shifted(e[x + 1], 2) + (field[p, x, here, :] + field[p, x + 4, here, :]))
                + vertical_weight * (up + down)
            )

    def fold(value):
        return functools.reduce(
            lambda s, t: s + t, [value[:, c : c + LANES] for c in range(0, width, LANES)]
        )

    to_partner.wait_recv()
    term = active * (shared[1] * shared[0])

    edge = jnp.where(is_ice, 0, layers - 1).astype(jnp.int32)

    def zeroth(c, acc):
        forward(chunks + c - lag)
        finish_recv(0, c)
        corners = blank
        for t in range(per):
            j = c * per + t
            ls = pl.ds(pl.multiple_of(j * SUB, SUB), SUB)
            layer = sub + j * SUB
            at_edge = layer == edge
            at_bottom = layer == 0
            tile = blank
            for x, around in enumerate(list(spread_block(0, c, t))):
                own = coupling[x, ls, :]
                diag = (
                    extra[x, ls, :] + jnp.where(at_bottom, wide(friction, x), 0.0) + own * around
                )
                inverse = 1.0 / diag
                source = wide(active, x) * force[x, ls, :] + jnp.where(at_edge, wide(term, x), 0.0)
                vector = inverse * source
                diagonal[x, ls, :] = diag
                scaled[x, ls, :] = inverse * own
                basis[0, x, ls, :] = zero
                basis[1, x, ls, :] = vector
                value = own * vector
                field[1, x + 2, pl.ds(pl.multiple_of(j * SUB + SUB, SUB), SUB), :] = value
                tile, corners = pack_row(x, value, tile, t, corners)
                acc = acc + source * vector
            pack[1, ls, :] = tile
        put_corner(1, c, corners)
        start(1, c, 1)
        return acc

    partial[0] = fold(lax.fori_loop(0, chunks, zeroth, zero))
    partial[1] = blank
    to_partner.wait_send()

    def step(k, carry):
        p = lax.rem(k, 2)
        q = 1 - p
        gain = jnp.where(k == 1, 1.0, 2.0).astype(jnp.float32)

        def block(c, accs):
            own_acc, cross_acc = accs
            message = (k + 1) * chunks + c - lag

            @pl.when(message < (ITERS + 1) * chunks)
            def _():
                forward(message)

            finish_recv(p, c)
            finish_send(q, c)
            corners = blank
            for t in range(per):
                j = c * per + t
                ls = pl.ds(pl.multiple_of(j * SUB, SUB), SUB)
                tile = blank
                vectors, values = [], []
                for x, around in enumerate(list(spread_block(p, c, t))):
                    vector = gain * (scaled[x, ls, :] * around) - basis[k - 1, x, ls, :]
                    weighted = diagonal[x, ls, :] * vector
                    value = coupling[x, ls, :] * vector
                    own_acc = own_acc + weighted * vector
                    cross_acc = cross_acc + weighted * basis[k, x, ls, :]
                    tile, corners = pack_row(x, value, tile, t, corners)
                    vectors.append(vector)
                    values.append(value)
                after = pl.ds(pl.multiple_of(j * SUB + SUB, SUB), SUB)
                for x in range(rows):
                    basis[k + 1, x, ls, :] = vectors[x]
                    field[q, x + 2, after, :] = values[x]
                pack[q, ls, :] = tile
            put_corner(q, c, corners)

            @pl.when(k < ITERS)
            def _():
                start(q, c, k + 1)

            return own_acc, cross_acc

        own_acc, cross_acc = lax.fori_loop(0, chunks, block, (zero, zero))
        partial[2 * k] = fold(own_acc)
        partial[2 * k + 1] = fold(cross_acc)
        return carry

    lax.fori_loop(1, ITERS + 1, step, 0)

    def settle(c, carry):
        finish_send(ITERS % 2, c)
        for path in detours:
            @pl.when((gx == path[1]) & relayed)
            def _():
                for p in range(2):
                    onward(path, p, c, 0).wait_send()
        return carry

    lax.fori_loop(0, chunks, settle, 0)

    count = 2 * ITERS + 2

    def total(own, slots, n, me, axis, sends, recvs):
        slots[me] = own
        copies = []
        for o in range(1, n):
            peer = lax.rem(me + o, n)
            device = (gg, peer, gy) if axis == "gx" else (gg, gx, peer)
            copy = pltpu.make_async_remote_copy(
                src_ref=slots.at[me],
                dst_ref=slots.at[me],
                send_sem=sends.at[o - 1],
                recv_sem=recvs.at[o - 1],
                device_id=device,
                device_id_type=pl.DeviceIdType.MESH,
            )
            copy.start()
            copies.append(copy)
        for copy in copies:
            copy.wait_recv()
        result = slots[0]
        for o in range(1, n):
            result = result + slots[o]
        for copy in copies:
            copy.wait_send()
        return result

    own = jnp.concatenate(
        [jnp.sum(partial[m], axis=0, keepdims=True) for m in range(count)]
        + [jnp.zeros((2 * SUB - count, LANES), jnp.float32)],
        axis=0,
    )
    own = total(own, sum_x, nx, gx, "gx", sx_send, sx_recv)
    own = total(own, sum_y, ny, gy, "gy", sy_send, sy_recv)
    sums = jnp.sum(own, axis=1, keepdims=True)
    dots = [jnp.broadcast_to(sums[m : m + 1, :], (SUB, LANES)) for m in range(count)]
    moments = [dots[0], dots[3]]
    for k in range(1, ITERS + 1):
        if k > 1:
            moments.append(2.0 * dots[2 * k + 1] - moments[1])
        moments.append(2.0 * dots[2 * k] - moments[0])
    iterate, left = coefficients(moments)

    def widen(value):
        return jnp.concatenate([value] * (width // LANES), axis=1)

    iterate, left = [widen(v) for v in iterate], [widen(v) for v in left]

    def last(j, carry):
        ls = pl.ds(pl.multiple_of(j * SUB, SUB), SUB)
        for x in range(rows):
            us = [basis[k + 1, x, ls, :] for k in range(ITERS + 1)]
            out_x[x, ls, :] = functools.reduce(
                lambda s, t: s + t, [a * u for a, u in zip(iterate, us)]
            )
            out_r[x, ls, :] = diagonal[x, ls, :] * functools.reduce(
                lambda s, t: s + t, [a * u for a, u in zip(left, us)]
            )
        return carry

    lax.fori_loop(0, tiles, last, 0)


def on_device(nx, ny, forcing, conduct, diag_add, ice_mask, grounded):
    def turned(a):
        return jnp.transpose(a[0].astype(jnp.float32), (1, 0, 2))

    _, layers, rows, width = forcing.shape
    tiles = layers // SUB
    chunks = tiles // next(t for t in CHUNK_TILES if tiles % t == 0)
    f32 = jnp.float32
    block = jax.ShapeDtypeStruct((rows, layers, width), f32)
    vmem = pl.BlockSpec(memory_space=pltpu.VMEM)
    dma = pltpu.SemaphoreType.DMA
    out_x, out_r = pl.pallas_call(
        functools.partial(kernel, (nx, ny)),
        out_shape=(block, block),
        in_specs=[vmem] * 5,
        out_specs=(vmem, vmem),
        scratch_shapes=[
            pltpu.VMEM((2, rows + 4, layers + 2 * SUB, width), f32),
            pltpu.VMEM((2, layers, LANES), f32),
            pltpu.VMEM((2, layers, LANES), f32),
            pltpu.VMEM((2, layers, LANES), f32),
            pltpu.VMEM((2, chunks, 1, LANES), f32),
            pltpu.VMEM((2, chunks, 4, 1, LANES), f32),
            pltpu.VMEM((ITERS + 1, 2, layers, width), f32),
            pltpu.VMEM((ITERS + 2, rows, layers, width), f32),
            pltpu.VMEM((rows, layers, width), f32),
            pltpu.VMEM((rows, layers, width), f32),
            pltpu.VMEM((rows, layers, width), f32),
            pltpu.VMEM((2, rows, width), f32),
            pltpu.VMEM((2, rows, width), f32),
            pltpu.VMEM((2 * ITERS + 2, SUB, LANES), f32),
            pltpu.VMEM((nx, 2 * SUB, LANES), f32),
            pltpu.VMEM((ny, 2 * SUB, LANES), f32),
            dma((2, chunks, 8)),
            dma((2, chunks, 8)),
            dma((2,)),
            dma((4, 2, chunks)),
            dma((nx - 1,)),
            dma((nx - 1,)),
            dma((ny - 1,)),
            dma((ny - 1,)),
        ],
        compiler_params=pltpu.CompilerParams(
            collective_id=0, has_side_effects=True, vmem_limit_bytes=40 * 1024 * 1024
        ),
        name="krylov",
    )(turned(forcing), turned(conduct), turned(diag_add), ice_mask, grounded)
    return tuple(jnp.transpose(o, (1, 0, 2))[None] for o in (out_x, out_r))


def solution(mesh):
    spec = P("group", None, "gx", "gy")
    flat = P("gx", "gy")
    return jax.shard_map(
        functools.partial(on_device, mesh.shape["gx"], mesh.shape["gy"]),
        mesh=mesh,
        in_specs=(spec, spec, spec, flat, flat),
        out_specs=(spec, spec),
        check_vma=False,
    )
```

```python
import functools

import jax
import jax.numpy as jnp
from jax import lax
from jax.experimental import pallas as pl
from jax.experimental.pallas import tpu as pltpu
from jax.sharding import PartitionSpec as P

ITERS = 6
far_weight = 0.25
cross_weight = 0.5
vertical_weight = 4.0
friction_gain = 8.0
SUB = 8
LANES = 128
CHUNK_TILES = (1,)


def coefficients(moments):
    def gram(j, k):
        return 0.5 * (moments[j + k] + moments[abs(j - k)])

    table = {
        (j, k): gram(j, k)
        for j in range(ITERS + 1)
        for k in range(j, ITERS + 1)
        if j + k < len(moments)
    }

    def form(a, b):
        terms = []
        for j in range(len(a)):
            row = None
            for k in range(len(b)):
                term = table[min(j, k), max(j, k)] * b[k]
                row = term if row is None else row + term
            terms.append(a[j] * row)
        return functools.reduce(lambda s, t: s + t, terms)

    def shift(e):
        out = [jnp.zeros_like(e[0]) for _ in range(len(e) + 1)]
        for k, value in enumerate(e):
            if k == 0:
                out[1] = out[1] + value
            else:
                out[k + 1] = out[k + 1] + 0.5 * value
                out[k - 1] = out[k - 1] + 0.5 * value
        return out

    left = [jnp.ones_like(moments[0])]
    direction = list(left)
    iterate = []
    norm_now = form(left, left)
    for iteration in range(ITERS):
        moved = shift(direction)
        applied = [
            (direction[k] - moved[k]) if k < len(direction) else -moved[k]
            for k in range(len(moved))
        ]
        if iteration + 1 == ITERS:
            table[iteration, ITERS] = 0.5 * moments[1]
            slope = 0.5 * direction[-1] * applied[-1]
            return iterate, left, direction, applied, norm_now, form(direction, applied), slope
        step = norm_now / form(direction, applied)
        iterate = [
            (iterate[k] if k < len(iterate) else 0.0) + step * direction[k]
            for k in range(len(direction))
        ]
        left = [
            (left[k] - step * applied[k]) if k < len(left) else -step * applied[k]
            for k in range(len(applied))
        ]
        norm_next = form(left, left)
        ratio = norm_next / norm_now
        direction = [
            left[k] + (ratio * direction[k] if k < len(direction) else 0.0)
            for k in range(len(left))
        ]
        norm_now = norm_next


def kernel(
    sizes,
    force_hbm,
    conduct,
    extra,
    ice,
    grounded,
    out_x,
    out_p,
    out_r,
    out_q,
    out_s,
    field,
    pack,
    rim_right,
    rim_left,
    corner,
    cornered,
    held,
    basis,
    coupling,
    scaled,
    diagonal,
    share,
    shared,
    partial,
    sum_early,
    sum_all,
    send_sem,
    recv_sem,
    share_sem,
    detour_sem,
    se_send,
    se_recv,
    sa_send,
    sa_recv,
    force,
    force_sem,
):
    nx, ny = sizes
    rows, layers, width = conduct.shape
    fetch = pltpu.make_async_copy(force_hbm, force, force_sem)
    fetch.start()
    tiles = layers // SUB
    chunks = corner.shape[1]
    per = tiles // chunks
    deep = per * SUB
    gg, gx, gy = lax.axis_index("group"), lax.axis_index("gx"), lax.axis_index("gy")
    is_ice = gg == 0

    def there(dx, dy):
        ok = None
        for d, g, n in ((dx, gx, nx), (dy, gy, ny)):
            if d != 0:
                one = (g + d >= 0) & (g + d < n)
                ok = one if ok is None else ok & one
        return ok

    def at(dx, dy):
        return (gg, gx + dx, gy + dy)

    two = 2 * rows
    sides = ((-1, 0), (1, 0), (0, -1), (0, 1), (-1, -1), (1, -1), (-1, 1), (1, 1))

    def copy_of(i, p, c, span=2):
        dx, dy = sides[i]
        inner = pl.ds(pl.multiple_of(c * deep + SUB, SUB), deep)
        flat = pl.ds(pl.multiple_of(c * deep, SUB), deep)
        if i == 0:
            source = field.at[p, 2 : 2 + span, inner]
            target = field.at[p, rows + 2 : rows + 2 + span, inner]
        elif i == 1:
            source = field.at[p, rows : rows + span, inner]
            target = field.at[p, 0:span, inner]
        elif i == 2:
            source, target = pack.at[p, flat], rim_right.at[p, flat]
        elif i == 3:
            source, target = pack.at[p, flat], rim_left.at[p, flat]
        else:
            source, target = corner.at[p, c], cornered.at[p, c, i - 4]
        return pltpu.make_async_remote_copy(
            src_ref=source,
            dst_ref=target,
            send_sem=send_sem.at[p, c, i],
            recv_sem=recv_sem.at[p, c, i],
            device_id=at(dx, dy),
            device_id_type=pl.DeviceIdType.MESH,
        )

    detours = ((1, 3, 2, rows, 0), (2, 0, 1, 2, rows + 2)) if nx == 4 else ()
    relayed = gg == 1
    lag = min(3, chunks - 1)

    def each(toward, act):
        for i, (dx, dy) in enumerate(sides):
            ok = there(toward * dx, toward * dy)
            if i < 2 and detours:
                split = gx == ((2 - i) if toward > 0 else (1 + i))

                ok = ok & jnp.logical_not(split & relayed)

            @pl.when(ok)
            def _():
                act(i, 2)

    def away(path, p, c, slot):
        origin, relay, _, row, _ = path
        return pltpu.make_async_remote_copy(
            src_ref=field.at[p, row : row + 2, pl.ds(pl.multiple_of(c * deep + SUB, SUB), deep)],
            dst_ref=held.at[slot, :, pl.ds(pl.multiple_of(c * deep, SUB), deep)],
            send_sem=detour_sem.at[0, p, c],
            recv_sem=detour_sem.at[1, p, c],
            device_id=(gg, relay, gy),
            device_id_type=pl.DeviceIdType.MESH,
        )

    def onward(path, p, c, slot):
        _, _, end, _, row = path
        return pltpu.make_async_remote_copy(
            src_ref=held.at[slot, :, pl.ds(pl.multiple_of(c * deep, SUB), deep)],
            dst_ref=field.at[p, row : row + 2, pl.ds(pl.multiple_of(c * deep + SUB, SUB), deep)],
            send_sem=detour_sem.at[2, p, c],
            recv_sem=detour_sem.at[3, p, c],
            device_id=(gg, end, gy),
            device_id_type=pl.DeviceIdType.MESH,
        )

    def forward(message):
        slot = message // chunks
        c = message % chunks
        p = slot % 2
        for path in detours:
            @pl.when((gx == path[1]) & relayed)
            def _():
                @pl.when(slot >= 2)
                def _():
                    onward(path, p, c, slot).wait_send()

                away(path, p, c, slot).wait_recv()
                onward(path, p, c, slot).start()

    def start(p, c, slot):
        for path in detours:
            @pl.when((gx == path[0]) & relayed)
            def _():
                away(path, p, c, slot).start()
        each(1, lambda i, span: copy_of(i, p, c, span).start())

    def finish_recv(p, c):
        for path in detours:
            @pl.when((gx == path[2]) & relayed)
            def _():
                onward(path, p, c, 0).wait_recv()
        each(-1, lambda i, span: copy_of(i, p, c, span).wait_recv())

    def finish_send(p, c):
        for path in detours:
            @pl.when((gx == path[0]) & relayed)
            def _():
                away(path, p, c, 0).wait_send()
        each(1, lambda i, span: copy_of(i, p, c, span).wait_send())

    for p in range(2):
        for r, d in ((0, -1), (rows + 2, 1)):
            @pl.when(jnp.logical_not(there(d, 0)))
            def _():
                field[p, r : r + 2] = jnp.zeros((2, layers + 2 * SUB, width), jnp.float32)
        for r in range(2, rows + 2):
            for s in (0, SUB + layers):
                field[p, r, s : s + SUB] = jnp.zeros((SUB, width), jnp.float32)
        for ref, d in ((rim_left, -1), (rim_right, 1)):
            @pl.when(jnp.logical_not(there(0, d)))
            def _():
                ref[p] = jnp.zeros(ref.shape[1:], jnp.float32)
        for i in range(4):
            @pl.when(jnp.logical_not(there(-sides[4 + i][0], -sides[4 + i][1])))
            def _():
                for c in range(chunks):
                    cornered[p, c, i] = jnp.zeros((1, LANES), jnp.float32)

    barrier = pltpu.get_barrier_semaphore()

    def peers_all():
        me = gx * ny + gy
        out = []
        for o in range(1, nx * ny):
            peer = lax.rem(me + o, nx * ny)
            out.append((gg, peer // ny, lax.rem(peer, ny)))
        return out

    def greet(device):
        pl.semaphore_signal(
            barrier, inc=1, device_id=device, device_id_type=pl.DeviceIdType.MESH
        )

    greet((1 - gg, gx, gy))
    if max(nx, ny) < ITERS:
        met = jnp.int32(1)
        for dx, dy in sides:
            @pl.when(there(dx, dy))
            def _():
                greet(at(dx, dy))
            met = met + jnp.where(there(dx, dy), 1, 0).astype(jnp.int32)
        for origin, relay, end, _, _ in detours:
            for one, other in ((origin, relay), (relay, end)):
                for here, peer in ((one, other), (other, one)):
                    if abs(here - peer) > 1:
                        @pl.when(gx == here)
                        def _():
                            greet((gg, peer, gy))
                        met = met + jnp.where(gx == here, 1, 0).astype(jnp.int32)
    else:
        for device in peers_all():
            greet(device)
        met = jnp.int32(nx * ny)

    lane = lax.broadcasted_iota(jnp.int32, (SUB, LANES), 1)
    sub = lax.broadcasted_iota(jnp.int32, (SUB, width), 0)

    tile_row = lax.broadcasted_iota(jnp.int32, (SUB, LANES), 0)

    def spot(i, t):
        return lane == (i * per + t) * SUB + tile_row

    def pack_row(x, value, tile, t, corners):
        first, last = value[:, :LANES], value[:, width - LANES :]
        low = first if x == 0 else pltpu.roll(first, 2 * x, 1)
        high = pltpu.roll(last, (two + 2 * x - LANES + 2) % LANES, 1)
        tile = jnp.where((lane >= 2 * x) & (lane < 2 * x + 2), low, tile)
        tile = jnp.where((lane >= two + 2 * x) & (lane < two + 2 * x + 2), high, tile)
        for i, (at_x, y) in enumerate(
            ((0, 0), (rows - 1, 0), (0, width - 1), (rows - 1, width - 1))
        ):
            if x == at_x:
                column = jnp.broadcast_to(value[:, y : y + 1], (SUB, LANES))
                corners = jnp.where(spot(i, t), column, corners)
        return tile, corners

    def put_corner(p, c, corners):
        corner[p, c] = jnp.sum(corners, axis=0, keepdims=True)

    ice_cells = ice[...].astype(jnp.float32)
    ground_cells = grounded[...].astype(jnp.float32)
    ocean = jnp.where(is_ice, 0.0, 1.0).astype(jnp.float32)
    active = ice_cells * (1.0 - ocean * ground_cells)
    friction = (1.0 - ocean) * friction_gain * ground_cells * ice_cells

    def wide(array, x):
        return jnp.broadcast_to(array[x : x + 1, :], (SUB, width))

    blank = jnp.zeros((SUB, LANES), jnp.float32)
    zero = jnp.zeros((SUB, width), jnp.float32)

    def first_pass(c, carry):
        @pl.when(c >= lag)
        def _():
            forward(c - lag)

        corners = blank
        for t in range(per):
            j = c * per + t
            ls = pl.ds(pl.multiple_of(j * SUB, SUB), SUB)
            tile = blank
            for x in range(rows):
                value = jnp.sqrt(conduct[x, ls, :]) * wide(active, x)
                coupling[x, ls, :] = value
                field[0, x + 2, pl.ds(pl.multiple_of(j * SUB + SUB, SUB), SUB), :] = value
                tile, corners = pack_row(x, value, tile, t, corners)
            pack[0, ls, :] = tile
        put_corner(0, c, corners)
        start(0, c, 0)
        return carry

    pl.semaphore_wait(barrier, met)
    lax.fori_loop(0, chunks, first_pass, 0)
    fetch.wait()

    def gather(j, total):
        for t in range(SUB):
            total = total + force[j * SUB + t]
        return total

    total = lax.fori_loop(0, tiles, gather, jnp.zeros((rows, width), jnp.float32))
    share[0] = active * (total * (1.0 / layers))
    for x in range(rows):
        share[1, x : x + 1, :] = jnp.where(
            is_ice, coupling[x, 0:1, :], coupling[x, layers - 1 : layers, :]
        )

    to_partner = pltpu.make_async_remote_copy(
        src_ref=share,
        dst_ref=shared,
        send_sem=share_sem.at[0],
        recv_sem=share_sem.at[1],
        device_id=(1 - gg, gx, gy),
        device_id_type=pl.DeviceIdType.MESH,
    )
    to_partner.start()

    def spread_block(p, c, t):
        j = c * per + t
        here = pl.ds(pl.multiple_of(j * SUB + SUB, SUB), SUB)
        below = pl.ds(pl.multiple_of(j * SUB, SUB), SUB)
        above = pl.ds(pl.multiple_of(j * SUB + 2 * SUB, SUB), SUB)
        from_right, from_left = rim_right[p, below, :], rim_left[p, below, :]

        def column(i):
            row = jnp.broadcast_to(cornered[p, c, i], (SUB, LANES))
            return jnp.sum(jnp.where(spot(i, t), row, 0.0), axis=1, keepdims=True)

        def rim(x):
            right = from_right if x == 0 else pltpu.roll(from_right, LANES - 2 * x, 1)
            left = pltpu.roll(from_left, (LANES - 2 - two - 2 * x) % LANES, 1)
            return jnp.where(lane < LANES // 2, right, left)

        def line(x):
            if x == 0:
                edge = jnp.where(lane < LANES // 2, column(1), column(3))
            elif x == rows + 1:
                edge = jnp.where(lane < LANES // 2, column(0), column(2))
            else:
                edge = rim(x - 1)
            value = field[p, x + 1, here, :]
            return [value[:, l : l + LANES] for l in range(0, width, LANES)] + [edge]

        def shifted(tiles_in, by):
            count = len(tiles_in) - 1
            out = []
            for i in range(count):
                before, own, after = tiles_in[i - 1], tiles_in[i], tiles_in[i + 1]
                up = pltpu.roll(jnp.where(lane >= LANES - by, before, own), by, 1)
                down = pltpu.roll(jnp.where(lane < by, after, own), LANES - by, 1)
                out.append(up + down)
            return jnp.concatenate(out, axis=1)

        e = [line(0), line(1)]
        for x in range(rows):
            e.append(line(x + 2))
            beside = [a + b for a, b in zip(e[x], e[x + 2])]
            h = [a + cross_weight * b for a, b in zip(e[x + 1], beside)]
            mine = field[p, x + 2, here, :]
            up = pltpu.roll(jnp.where(sub == 0, field[p, x + 2, above, :], mine), SUB - 1, 0)
            down = pltpu.roll(jnp.where(sub == SUB - 1, field[p, x + 2, below, :], mine), 1, 0)
            yield (
                shifted(h, 1)
                + jnp.concatenate(beside[:-1], axis=1)
                + far_weight
                * (shifted(e[x + 1], 2) + (field[p, x, here, :] + field[p, x + 4, here, :]))
                + vertical_weight * (up + down)
            )

    def fold(value):
        return functools.reduce(
            lambda s, t: s + t, [value[:, c : c + LANES] for c in range(0, width, LANES)]
        )

    to_partner.wait_recv()
    term = active * (shared[1] * shared[0])

    edge = jnp.where(is_ice, 0, layers - 1).astype(jnp.int32)

    def zeroth(c, acc):
        forward(chunks + c - lag)
        finish_recv(0, c)
        corners = blank
        for t in range(per):
            j = c * per + t
            ls = pl.ds(pl.multiple_of(j * SUB, SUB), SUB)
            layer = sub + j * SUB
            at_edge = layer == edge
            at_bottom = layer == 0
            tile = blank
            for x, around in enumerate(list(spread_block(0, c, t))):
                own = coupling[x, ls, :]
                diag = (
                    extra[x, ls, :] + jnp.where(at_bottom, wide(friction, x), 0.0) + own * around
                )
                inverse = 1.0 / diag
                source = wide(active, x) * force[ls, x, :] + jnp.where(at_edge, wide(term, x), 0.0)
                vector = inverse * source
                diagonal[x, ls, :] = diag
                scaled[x, ls, :] = inverse * own
                basis[0, x, ls, :] = zero
                basis[1, x, ls, :] = vector
                value = own * vector
                field[1, x + 2, pl.ds(pl.multiple_of(j * SUB + SUB, SUB), SUB), :] = value
                tile, corners = pack_row(x, value, tile, t, corners)
                acc = acc + source * vector
            pack[1, ls, :] = tile
        put_corner(1, c, corners)
        start(1, c, 1)
        return acc

    partial[0] = fold(lax.fori_loop(0, chunks, zeroth, zero))
    partial[1] = blank
    to_partner.wait_send()

    lane_row = lax.broadcasted_iota(jnp.int32, (1, LANES), 1)

    def copies(slots, me, devices, sends, recvs):
        return [
            pltpu.make_async_remote_copy(
                src_ref=slots.at[me],
                dst_ref=slots.at[me],
                send_sem=sends.at[o],
                recv_sem=recvs.at[o],
                device_id=device,
                device_id_type=pl.DeviceIdType.MESH,
            )
            for o, device in enumerate(devices)
        ]

    def row_of(slots):
        return functools.reduce(lambda s, t: s + t, [slots[o] for o in range(slots.shape[0])])

    def copies_early():
        return copies(sum_early, gx * ny + gy, peers_all(), se_send, se_recv)

    def early_start():
        row = jnp.zeros((1, LANES), jnp.float32)
        for m in range(2 * ITERS):
            value = jnp.sum(partial[m], axis=0, keepdims=True)
            value = jnp.sum(value, axis=1, keepdims=True)
            row = jnp.where(lane_row == m, jnp.broadcast_to(value, (1, LANES)), row)
        sum_early[gx * ny + gy] = row
        for copy in copies_early():
            copy.start()

    def early_finish():
        for copy in copies_early():
            copy.wait_recv()
        for copy in copies_early():
            copy.wait_send()

    def step(k, carry):
        p = lax.rem(k, 2)
        q = 1 - p
        gain = jnp.where(k == 1, 1.0, 2.0).astype(jnp.float32)

        def block(c, accs):
            own_acc, cross_acc = accs
            message = (k + 1) * chunks + c - lag

            @pl.when(message < (ITERS + 1) * chunks)
            def _():
                forward(message)

            finish_recv(p, c)
            finish_send(q, c)
            corners = blank
            for t in range(per):
                j = c * per + t
                ls = pl.ds(pl.multiple_of(j * SUB, SUB), SUB)
                tile = blank
                vectors, values = [], []
                for x, around in enumerate(list(spread_block(p, c, t))):
                    vector = gain * (scaled[x, ls, :] * around) - basis[k - 1, x, ls, :]
                    weighted = diagonal[x, ls, :] * vector
                    value = coupling[x, ls, :] * vector
                    own_acc = own_acc + weighted * vector
                    cross_acc = cross_acc + weighted * basis[k, x, ls, :]
                    tile, corners = pack_row(x, value, tile, t, corners)
                    vectors.append(vector)
                    values.append(value)
                after = pl.ds(pl.multiple_of(j * SUB + SUB, SUB), SUB)
                for x in range(rows):
                    basis[k + 1, x, ls, :] = vectors[x]
                    field[q, x + 2, after, :] = values[x]
                pack[q, ls, :] = tile
            put_corner(q, c, corners)

            @pl.when(k < ITERS)
            def _():
                start(q, c, k + 1)

            return own_acc, cross_acc

        own_acc, cross_acc = lax.fori_loop(0, chunks, block, (zero, zero))
        partial[2 * k] = fold(own_acc)
        partial[2 * k + 1] = fold(cross_acc)

        @pl.when(k == ITERS - 1)
        def _():
            early_start()

        return carry

    lax.fori_loop(1, ITERS + 1, step, 0)
    sum_all[gx * ny + gy] = jnp.sum(partial[2 * ITERS + 1], axis=0, keepdims=True)
    to_all = copies(sum_all, gx * ny + gy, peers_all(), sa_send, sa_recv)
    for copy in to_all:
        copy.start()

    def settle(c, carry):
        finish_send(ITERS % 2, c)
        for path in detours:
            @pl.when((gx == path[1]) & relayed)
            def _():
                for p in range(2):
                    onward(path, p, c, 0).wait_send()
        return carry

    lax.fori_loop(0, chunks, settle, 0)

    early_finish()
    total = row_of(sum_early)
    dots = [jnp.broadcast_to(total[:, m : m + 1], (SUB, LANES)) for m in range(2 * ITERS)]
    moments = [dots[0], dots[3]]
    for k in range(1, ITERS):
        if k > 1:
            moments.append(2.0 * dots[2 * k + 1] - moments[1])
        moments.append(2.0 * dots[2 * k] - moments[0])
    *lists, norm, fixed, slope = coefficients(moments)

    def widen(value):
        return jnp.concatenate([value] * (width // LANES), axis=1)

    iterate, left, direction, applied = [[widen(v) for v in values] for values in lists]

    def combined(values, us):
        return functools.reduce(lambda s, t: s + t, [a * u for a, u in zip(values, us)])

    def last(j, carry):
        ls = pl.ds(pl.multiple_of(j * SUB, SUB), SUB)
        for x in range(rows):
            us = [basis[k + 1, x, ls, :] for k in range(ITERS + 1)]
            diag = diagonal[x, ls, :]
            out_x[ls, x, :] = combined(iterate, us)
            out_p[ls, x, :] = combined(direction, us)
            out_r[ls, x, :] = diag * combined(left, us)
            out_q[ls, x, :] = diag * combined(applied, us)
        return carry

    lax.fori_loop(0, tiles, last, 0)

    for copy in to_all:
        copy.wait_recv()
    cross = jnp.sum(row_of(sum_all), axis=1, keepdims=True)
    cross = jnp.broadcast_to(cross, (SUB, LANES))
    out_s[...] = widen(norm / (fixed + slope * (2.0 * cross - moments[1])))
    for copy in to_all:
        copy.wait_send()


def on_device(nx, ny, forcing, conduct, diag_add, ice_mask, grounded):
    def turned(a):
        return jnp.transpose(a[0].astype(jnp.float32), (1, 0, 2))

    _, layers, rows, width = forcing.shape
    tiles = layers // SUB
    chunks = tiles // next(t for t in CHUNK_TILES if tiles % t == 0)
    f32 = jnp.float32
    block = jax.ShapeDtypeStruct((rows, layers, width), f32)
    vmem = pl.BlockSpec(memory_space=pltpu.VMEM)
    dma = pltpu.SemaphoreType.DMA
    out_x, out_p, out_r, out_q, out_s = pl.pallas_call(
        functools.partial(kernel, (nx, ny)),
        out_shape=(jax.ShapeDtypeStruct((layers, rows, width), f32),) * 4 + (jax.ShapeDtypeStruct((SUB, width), f32),),
        in_specs=[pl.BlockSpec(memory_space=pl.ANY)] + [vmem] * 4,
        out_specs=(vmem,) * 5,
        scratch_shapes=[
            pltpu.VMEM((2, rows + 4, layers + 2 * SUB, width), f32),
            pltpu.VMEM((2, layers, LANES), f32),
            pltpu.VMEM((2, layers, LANES), f32),
            pltpu.VMEM((2, layers, LANES), f32),
            pltpu.VMEM((2, chunks, 1, LANES), f32),
            pltpu.VMEM((2, chunks, 4, 1, LANES), f32),
            pltpu.VMEM((ITERS + 1, 2, layers, width), f32),
            pltpu.VMEM((ITERS + 2, rows, layers, width), f32),
            pltpu.VMEM((rows, layers, width), f32),
            pltpu.VMEM((rows, layers, width), f32),
            pltpu.VMEM((rows, layers, width), f32),
            pltpu.VMEM((2, rows, width), f32),
            pltpu.VMEM((2, rows, width), f32),
            pltpu.VMEM((2 * ITERS + 2, SUB, LANES), f32),
            pltpu.VMEM((nx * ny, 1, LANES), f32),
            pltpu.VMEM((nx * ny, 1, LANES), f32),
            dma((2, chunks, 8)),
            dma((2, chunks, 8)),
            dma((2,)),
            dma((4, 2, chunks)),
            dma((nx * ny - 1,)),
            dma((nx * ny - 1,)),
            dma((nx * ny - 1,)),
            dma((nx * ny - 1,)),
            pltpu.VMEM((layers, rows, width), f32),
            dma,
        ],
        compiler_params=pltpu.CompilerParams(
            collective_id=0, has_side_effects=True, vmem_limit_bytes=40 * 1024 * 1024
        ),
        name="krylov",
    )(forcing[0], turned(conduct), turned(diag_add), ice_mask, grounded)
    step = out_s[:1]
    solved, residual = out_x + step * out_p, out_r - step * out_q
    return tuple(o[None] for o in (solved, residual))


def solution(mesh):
    spec = P("group", None, "gx", "gy")
    flat = P("gx", "gy")
    return jax.shard_map(
        functools.partial(on_device, mesh.shape["gx"], mesh.shape["gy"]),
        mesh=mesh,
        in_specs=(spec, spec, spec, flat, flat),
        out_specs=(spec, spec),
        check_vma=False,
    )
```

```python
import functools

import jax
import jax.numpy as jnp
from jax import lax
from jax.experimental import pallas as pl
from jax.experimental.pallas import tpu as pltpu
from jax.sharding import PartitionSpec as P

ITERS = 6
far_weight = 0.25
cross_weight = 0.5
vertical_weight = 4.0
friction_gain = 8.0
SUB = 8
LANES = 128
CHUNK_TILES = (2, 1)


def coefficients(moments):
    def gram(j, k):
        return 0.5 * (moments[j + k] + moments[abs(j - k)])

    table = {
        (j, k): gram(j, k)
        for j in range(ITERS + 1)
        for k in range(j, ITERS + 1)
        if j + k < len(moments)
    }

    def form(a, b):
        terms = []
        for j in range(len(a)):
            row = None
            for k in range(len(b)):
                term = table[min(j, k), max(j, k)] * b[k]
                row = term if row is None else row + term
            terms.append(a[j] * row)
        return functools.reduce(lambda s, t: s + t, terms)

    def shift(e):
        out = [jnp.zeros_like(e[0]) for _ in range(len(e) + 1)]
        for k, value in enumerate(e):
            if k == 0:
                out[1] = out[1] + value
            else:
                out[k + 1] = out[k + 1] + 0.5 * value
                out[k - 1] = out[k - 1] + 0.5 * value
        return out

    left = [jnp.ones_like(moments[0])]
    direction = list(left)
    iterate = []
    norm_now = form(left, left)
    for iteration in range(ITERS):
        moved = shift(direction)
        applied = [
            (direction[k] - moved[k]) if k < len(direction) else -moved[k]
            for k in range(len(moved))
        ]
        if iteration + 1 == ITERS:
            table[iteration, ITERS] = 0.5 * moments[1]
            slope = 0.5 * direction[-1] * applied[-1]
            return iterate, left, direction, applied, norm_now, form(direction, applied), slope
        step = norm_now / form(direction, applied)
        iterate = [
            (iterate[k] if k < len(iterate) else 0.0) + step * direction[k]
            for k in range(len(direction))
        ]
        left = [
            (left[k] - step * applied[k]) if k < len(left) else -step * applied[k]
            for k in range(len(applied))
        ]
        norm_next = form(left, left)
        ratio = norm_next / norm_now
        direction = [
            left[k] + (ratio * direction[k] if k < len(direction) else 0.0)
            for k in range(len(left))
        ]
        norm_now = norm_next


def kernel(
    sizes,
    force,
    conduct,
    extra,
    ice,
    grounded,
    out_x,
    out_p,
    out_r,
    out_q,
    out_s,
    field,
    pack,
    rim_right,
    rim_left,
    corner,
    cornered,
    held,
    basis,
    coupling,
    scaled,
    diagonal,
    share,
    shared,
    partial,
    sum_early,
    sum_all,
    send_sem,
    recv_sem,
    share_sem,
    detour_sem,
    se_send,
    se_recv,
    sa_send,
    sa_recv,
):
    nx, ny = sizes
    rows, layers, width = conduct.shape
    tiles = layers // SUB
    chunks = corner.shape[1]
    per = tiles // chunks
    deep = per * SUB
    gg, gx, gy = lax.axis_index("group"), lax.axis_index("gx"), lax.axis_index("gy")
    is_ice = gg == 0

    def there(dx, dy):
        ok = None
        for d, g, n in ((dx, gx, nx), (dy, gy, ny)):
            if d != 0:
                one = (g + d >= 0) & (g + d < n)
                ok = one if ok is None else ok & one
        return ok

    def at(dx, dy):
        return (gg, gx + dx, gy + dy)

    two = 2 * rows
    sides = ((-1, 0), (1, 0), (0, -1), (0, 1), (-1, -1), (1, -1), (-1, 1), (1, 1))

    def copy_of(i, p, c, span=2):
        dx, dy = sides[i]
        inner = pl.ds(pl.multiple_of(c * deep + SUB, SUB), deep)
        flat = pl.ds(pl.multiple_of(c * deep, SUB), deep)
        if i == 0:
            source = field.at[p, 2 : 2 + span, inner]
            target = field.at[p, rows + 2 : rows + 2 + span, inner]
        elif i == 1:
            source = field.at[p, rows : rows + span, inner]
            target = field.at[p, 0:span, inner]
        elif i == 2:
            source, target = pack.at[p, flat], rim_right.at[p, flat]
        elif i == 3:
            source, target = pack.at[p, flat], rim_left.at[p, flat]
        else:
            source, target = corner.at[p, c], cornered.at[p, c, i - 4]
        return pltpu.make_async_remote_copy(
            src_ref=source,
            dst_ref=target,
            send_sem=send_sem.at[p, c, i],
            recv_sem=recv_sem.at[p, c, i],
            device_id=at(dx, dy),
            device_id_type=pl.DeviceIdType.MESH,
        )

    detours = ((1, 3, 2, rows, 0), (2, 0, 1, 2, rows + 2)) if nx == 4 else ()
    relayed = gg == 1
    lag = min(3, chunks - 1)

    def each(toward, act):
        for i, (dx, dy) in enumerate(sides):
            ok = there(toward * dx, toward * dy)
            if i < 2 and detours:
                split = gx == ((2 - i) if toward > 0 else (1 + i))

                ok = ok & jnp.logical_not(split & relayed)

            @pl.when(ok)
            def _():
                act(i, 2)

    def away(path, p, c, slot):
        origin, relay, _, row, _ = path
        return pltpu.make_async_remote_copy(
            src_ref=field.at[p, row : row + 2, pl.ds(pl.multiple_of(c * deep + SUB, SUB), deep)],
            dst_ref=held.at[slot, :, pl.ds(pl.multiple_of(c * deep, SUB), deep)],
            send_sem=detour_sem.at[0, p, c],
            recv_sem=detour_sem.at[1, p, c],
            device_id=(gg, relay, gy),
            device_id_type=pl.DeviceIdType.MESH,
        )

    def onward(path, p, c, slot):
        _, _, end, _, row = path
        return pltpu.make_async_remote_copy(
            src_ref=held.at[slot, :, pl.ds(pl.multiple_of(c * deep, SUB), deep)],
            dst_ref=field.at[p, row : row + 2, pl.ds(pl.multiple_of(c * deep + SUB, SUB), deep)],
            send_sem=detour_sem.at[2, p, c],
            recv_sem=detour_sem.at[3, p, c],
            device_id=(gg, end, gy),
            device_id_type=pl.DeviceIdType.MESH,
        )

    def forward(message):
        slot = message // chunks
        c = message % chunks
        p = slot % 2
        for path in detours:
            @pl.when((gx == path[1]) & relayed)
            def _():
                @pl.when(slot >= 2)
                def _():
                    onward(path, p, c, slot).wait_send()

                away(path, p, c, slot).wait_recv()
                onward(path, p, c, slot).start()

    def start(p, c, slot):
        for path in detours:
            @pl.when((gx == path[0]) & relayed)
            def _():
                away(path, p, c, slot).start()
        each(1, lambda i, span: copy_of(i, p, c, span).start())

    def finish_recv(p, c):
        for path in detours:
            @pl.when((gx == path[2]) & relayed)
            def _():
                onward(path, p, c, 0).wait_recv()
        each(-1, lambda i, span: copy_of(i, p, c, span).wait_recv())

    def finish_send(p, c):
        for path in detours:
            @pl.when((gx == path[0]) & relayed)
            def _():
                away(path, p, c, 0).wait_send()
        each(1, lambda i, span: copy_of(i, p, c, span).wait_send())

    barrier = pltpu.get_barrier_semaphore()

    def peers_all():
        me = gx * ny + gy
        out = []
        for o in range(1, nx * ny):
            peer = lax.rem(me + o, nx * ny)
            out.append((gg, peer // ny, lax.rem(peer, ny)))
        return out

    def greet(device):
        pl.semaphore_signal(
            barrier, inc=1, device_id=device, device_id_type=pl.DeviceIdType.MESH
        )

    greet((1 - gg, gx, gy))
    if max(nx, ny) < ITERS:
        met = jnp.int32(1)
        for dx, dy in sides:
            @pl.when(there(dx, dy))
            def _():
                greet(at(dx, dy))
            met = met + jnp.where(there(dx, dy), 1, 0).astype(jnp.int32)
        for origin, relay, end, _, _ in detours:
            for one, other in ((origin, relay), (relay, end)):
                for here, peer in ((one, other), (other, one)):
                    if abs(here - peer) > 1:
                        @pl.when(gx == here)
                        def _():
                            greet((gg, peer, gy))
                        met = met + jnp.where(gx == here, 1, 0).astype(jnp.int32)
    else:
        for device in peers_all():
            greet(device)
        met = jnp.int32(nx * ny)

    for p in range(2):
        for r, d in ((0, -1), (rows + 2, 1)):
            @pl.when(jnp.logical_not(there(d, 0)))
            def _():
                field[p, r : r + 2] = jnp.zeros((2, layers + 2 * SUB, width), jnp.float32)
        for r in range(2, rows + 2):
            for s in (0, SUB + layers):
                field[p, r, s : s + SUB] = jnp.zeros((SUB, width), jnp.float32)
        for ref, d in ((rim_left, -1), (rim_right, 1)):
            @pl.when(jnp.logical_not(there(0, d)))
            def _():
                ref[p] = jnp.zeros(ref.shape[1:], jnp.float32)
        for i in range(4):
            @pl.when(jnp.logical_not(there(-sides[4 + i][0], -sides[4 + i][1])))
            def _():
                for c in range(chunks):
                    cornered[p, c, i] = jnp.zeros((1, LANES), jnp.float32)

    lane = lax.broadcasted_iota(jnp.int32, (SUB, LANES), 1)
    sub = lax.broadcasted_iota(jnp.int32, (SUB, width), 0)

    tile_row = lax.broadcasted_iota(jnp.int32, (SUB, LANES), 0)

    def spot(i, t):
        return lane == (i * per + t) * SUB + tile_row

    def pack_row(x, value, tile, t, corners):
        first, last = value[:, :LANES], value[:, width - LANES :]
        low = first if x == 0 else pltpu.roll(first, 2 * x, 1)
        high = pltpu.roll(last, (two + 2 * x - LANES + 2) % LANES, 1)
        tile = jnp.where((lane >= 2 * x) & (lane < 2 * x + 2), low, tile)
        tile = jnp.where((lane >= two + 2 * x) & (lane < two + 2 * x + 2), high, tile)
        for i, (at_x, y) in enumerate(
            ((0, 0), (rows - 1, 0), (0, width - 1), (rows - 1, width - 1))
        ):
            if x == at_x:
                column = jnp.broadcast_to(value[:, y : y + 1], (SUB, LANES))
                corners = jnp.where(spot(i, t), column, corners)
        return tile, corners

    def put_corner(p, c, corners):
        corner[p, c] = jnp.sum(corners, axis=0, keepdims=True)

    ice_cells = ice[...].astype(jnp.float32)
    ground_cells = grounded[...].astype(jnp.float32)
    ocean = jnp.where(is_ice, 0.0, 1.0).astype(jnp.float32)
    active = ice_cells * (1.0 - ocean * ground_cells)
    friction = (1.0 - ocean) * friction_gain * ground_cells * ice_cells

    def wide(array, x):
        return jnp.broadcast_to(array[x : x + 1, :], (SUB, width))

    blank = jnp.zeros((SUB, LANES), jnp.float32)
    zero = jnp.zeros((SUB, width), jnp.float32)

    def first_pass(c, carry):
        @pl.when(c >= lag)
        def _():
            forward(c - lag)

        corners = blank
        for t in range(per):
            j = c * per + t
            ls = pl.ds(pl.multiple_of(j * SUB, SUB), SUB)
            tile = blank
            for x in range(rows):
                value = jnp.sqrt(conduct[x, ls, :]) * wide(active, x)
                coupling[x, ls, :] = value
                field[0, x + 2, pl.ds(pl.multiple_of(j * SUB + SUB, SUB), SUB), :] = value
                tile, corners = pack_row(x, value, tile, t, corners)
            pack[0, ls, :] = tile
        put_corner(0, c, corners)
        start(0, c, 0)
        return carry

    pl.semaphore_wait(barrier, met)
    lax.fori_loop(0, chunks, first_pass, 0)

    def gather(j, total):
        for t in range(SUB):
            total = total + force[j * SUB + t]
        return total

    total = lax.fori_loop(0, tiles, gather, jnp.zeros((rows, width), jnp.float32))
    share[0] = active * (total * (1.0 / layers))
    for x in range(rows):
        share[1, x : x + 1, :] = jnp.where(
            is_ice, coupling[x, 0:1, :], coupling[x, layers - 1 : layers, :]
        )

    to_partner = pltpu.make_async_remote_copy(
        src_ref=share,
        dst_ref=shared,
        send_sem=share_sem.at[0],
        recv_sem=share_sem.at[1],
        device_id=(1 - gg, gx, gy),
        device_id_type=pl.DeviceIdType.MESH,
    )
    to_partner.start()

    def spread_block(p, c, t):
        j = c * per + t
        here = pl.ds(pl.multiple_of(j * SUB + SUB, SUB), SUB)
        below = pl.ds(pl.multiple_of(j * SUB, SUB), SUB)
        above = pl.ds(pl.multiple_of(j * SUB + 2 * SUB, SUB), SUB)
        from_right, from_left = rim_right[p, below, :], rim_left[p, below, :]

        def column(i):
            row = jnp.broadcast_to(cornered[p, c, i], (SUB, LANES))
            return jnp.sum(jnp.where(spot(i, t), row, 0.0), axis=1, keepdims=True)

        def rim(x):
            right = from_right if x == 0 else pltpu.roll(from_right, LANES - 2 * x, 1)
            left = pltpu.roll(from_left, (LANES - 2 - two - 2 * x) % LANES, 1)
            return jnp.where(lane < LANES // 2, right, left)

        def line(x):
            if x == 0:
                edge = jnp.where(lane < LANES // 2, column(1), column(3))
            elif x == rows + 1:
                edge = jnp.where(lane < LANES // 2, column(0), column(2))
            else:
                edge = rim(x - 1)
            value = field[p, x + 1, here, :]
            return [value[:, l : l + LANES] for l in range(0, width, LANES)] + [edge]

        def shifted(tiles_in, by):
            count = len(tiles_in) - 1
            out = []
            for i in range(count):
                before, own, after = tiles_in[i - 1], tiles_in[i], tiles_in[i + 1]
                up = pltpu.roll(jnp.where(lane >= LANES - by, before, own), by, 1)
                down = pltpu.roll(jnp.where(lane < by, after, own), LANES - by, 1)
                out.append(up + down)
            return jnp.concatenate(out, axis=1)

        e = [line(0), line(1)]
        for x in range(rows):
            e.append(line(x + 2))
            beside = [a + b for a, b in zip(e[x], e[x + 2])]
            h = [a + cross_weight * b for a, b in zip(e[x + 1], beside)]
            mine = field[p, x + 2, here, :]
            up = pltpu.roll(jnp.where(sub == 0, field[p, x + 2, above, :], mine), SUB - 1, 0)
            down = pltpu.roll(jnp.where(sub == SUB - 1, field[p, x + 2, below, :], mine), 1, 0)
            yield (
                shifted(h, 1)
                + jnp.concatenate(beside[:-1], axis=1)
                + far_weight
                * (shifted(e[x + 1], 2) + (field[p, x, here, :] + field[p, x + 4, here, :]))
                + vertical_weight * (up + down)
            )

    def fold(value):
        return functools.reduce(
            lambda s, t: s + t, [value[:, c : c + LANES] for c in range(0, width, LANES)]
        )

    to_partner.wait_recv()
    term = active * (shared[1] * shared[0])

    edge = jnp.where(is_ice, 0, layers - 1).astype(jnp.int32)

    def zeroth(c, acc):
        forward(chunks + c - lag)
        finish_recv(0, c)
        corners = blank
        for t in range(per):
            j = c * per + t
            ls = pl.ds(pl.multiple_of(j * SUB, SUB), SUB)
            layer = sub + j * SUB
            at_edge = layer == edge
            at_bottom = layer == 0
            tile = blank
            for x, around in enumerate(list(spread_block(0, c, t))):
                own = coupling[x, ls, :]
                diag = (
                    extra[x, ls, :] + jnp.where(at_bottom, wide(friction, x), 0.0) + own * around
                )
                inverse = 1.0 / diag
                source = wide(active, x) * force[ls, x, :] + jnp.where(at_edge, wide(term, x), 0.0)
                vector = inverse * source
                diagonal[x, ls, :] = diag
                scaled[x, ls, :] = inverse * own
                basis[0, x, ls, :] = zero
                basis[1, x, ls, :] = vector
                value = own * vector
                field[1, x + 2, pl.ds(pl.multiple_of(j * SUB + SUB, SUB), SUB), :] = value
                tile, corners = pack_row(x, value, tile, t, corners)
                acc = acc + source * vector
            pack[1, ls, :] = tile
        put_corner(1, c, corners)
        start(1, c, 1)
        return acc

    partial[0] = fold(lax.fori_loop(0, chunks, zeroth, zero))
    partial[1] = blank
    to_partner.wait_send()

    lane_row = lax.broadcasted_iota(jnp.int32, (1, LANES), 1)

    def copies(slots, me, devices, sends, recvs):
        return [
            pltpu.make_async_remote_copy(
                src_ref=slots.at[me],
                dst_ref=slots.at[me],
                send_sem=sends.at[o],
                recv_sem=recvs.at[o],
                device_id=device,
                device_id_type=pl.DeviceIdType.MESH,
            )
            for o, device in enumerate(devices)
        ]

    def row_of(slots):
        return functools.reduce(lambda s, t: s + t, [slots[o] for o in range(slots.shape[0])])

    def copies_early():
        return copies(sum_early, gx * ny + gy, peers_all(), se_send, se_recv)

    def early_start():
        row = jnp.zeros((1, LANES), jnp.float32)
        for m in range(2 * ITERS):
            value = jnp.sum(partial[m], axis=0, keepdims=True)
            value = jnp.sum(value, axis=1, keepdims=True)
            row = jnp.where(lane_row == m, jnp.broadcast_to(value, (1, LANES)), row)
        sum_early[gx * ny + gy] = row
        for copy in copies_early():
            copy.start()

    def early_finish():
        for copy in copies_early():
            copy.wait_recv()
        for copy in copies_early():
            copy.wait_send()

    def step(k, carry):
        p = lax.rem(k, 2)
        q = 1 - p
        gain = jnp.where(k == 1, 1.0, 2.0).astype(jnp.float32)

        def block(c, accs):
            own_acc, cross_acc = accs
            message = (k + 1) * chunks + c - lag

            @pl.when(message < (ITERS + 1) * chunks)
            def _():
                forward(message)

            finish_recv(p, c)
            finish_send(q, c)
            corners = blank
            for t in range(per):
                j = c * per + t
                ls = pl.ds(pl.multiple_of(j * SUB, SUB), SUB)
                tile = blank
                vectors, values = [], []
                for x, around in enumerate(list(spread_block(p, c, t))):
                    vector = gain * (scaled[x, ls, :] * around) - basis[k - 1, x, ls, :]
                    weighted = diagonal[x, ls, :] * vector
                    value = coupling[x, ls, :] * vector
                    own_acc = own_acc + weighted * vector
                    cross_acc = cross_acc + weighted * basis[k, x, ls, :]
                    tile, corners = pack_row(x, value, tile, t, corners)
                    vectors.append(vector)
                    values.append(value)
                after = pl.ds(pl.multiple_of(j * SUB + SUB, SUB), SUB)
                for x in range(rows):
                    basis[k + 1, x, ls, :] = vectors[x]
                    field[q, x + 2, after, :] = values[x]
                pack[q, ls, :] = tile
            put_corner(q, c, corners)

            @pl.when(k < ITERS)
            def _():
                start(q, c, k + 1)

            return own_acc, cross_acc

        own_acc, cross_acc = lax.fori_loop(0, chunks, block, (zero, zero))
        partial[2 * k] = fold(own_acc)
        partial[2 * k + 1] = fold(cross_acc)

        @pl.when(k == ITERS - 1)
        def _():
            early_start()

        return carry

    lax.fori_loop(1, ITERS + 1, step, 0)
    sum_all[gx * ny + gy] = jnp.sum(partial[2 * ITERS + 1], axis=0, keepdims=True)
    to_all = copies(sum_all, gx * ny + gy, peers_all(), sa_send, sa_recv)
    for copy in to_all:
        copy.start()

    def settle(c, carry):
        finish_send(ITERS % 2, c)
        for path in detours:
            @pl.when((gx == path[1]) & relayed)
            def _():
                for p in range(2):
                    onward(path, p, c, 0).wait_send()
        return carry

    lax.fori_loop(0, chunks, settle, 0)

    early_finish()
    total = row_of(sum_early)
    dots = [jnp.broadcast_to(total[:, m : m + 1], (SUB, LANES)) for m in range(2 * ITERS)]
    moments = [dots[0], dots[3]]
    for k in range(1, ITERS):
        if k > 1:
            moments.append(2.0 * dots[2 * k + 1] - moments[1])
        moments.append(2.0 * dots[2 * k] - moments[0])
    *lists, norm, fixed, slope = coefficients(moments)

    def widen(value):
        return jnp.concatenate([value] * (width // LANES), axis=1)

    iterate, left, direction, applied = [[widen(v) for v in values] for values in lists]

    def combined(values, us):
        return functools.reduce(lambda s, t: s + t, [a * u for a, u in zip(values, us)])

    def last(j, carry):
        ls = pl.ds(pl.multiple_of(j * SUB, SUB), SUB)
        for x in range(rows):
            us = [basis[k + 1, x, ls, :] for k in range(ITERS + 1)]
            diag = diagonal[x, ls, :]
            out_x[ls, x, :] = combined(iterate, us)
            out_p[ls, x, :] = combined(direction, us)
            out_r[ls, x, :] = diag * combined(left, us)
            out_q[ls, x, :] = diag * combined(applied, us)
        return carry

    lax.fori_loop(0, tiles, last, 0)

    for copy in to_all:
        copy.wait_recv()
    cross = jnp.sum(row_of(sum_all), axis=1, keepdims=True)
    cross = jnp.broadcast_to(cross, (SUB, LANES))
    out_s[...] = widen(norm / (fixed + slope * (2.0 * cross - moments[1])))
    for copy in to_all:
        copy.wait_send()


def on_device(nx, ny, forcing, conduct, diag_add, ice_mask, grounded):
    def turned(a):
        return jnp.transpose(a[0].astype(jnp.float32), (1, 0, 2))

    _, layers, rows, width = forcing.shape
    tiles = layers // SUB
    chunks = tiles // next(t for t in CHUNK_TILES if tiles % t == 0)
    f32 = jnp.float32
    block = jax.ShapeDtypeStruct((rows, layers, width), f32)
    vmem = pl.BlockSpec(memory_space=pltpu.VMEM)
    dma = pltpu.SemaphoreType.DMA
    out_x, out_p, out_r, out_q, out_s = pl.pallas_call(
        functools.partial(kernel, (nx, ny)),
        out_shape=(jax.ShapeDtypeStruct((layers, rows, width), f32),) * 4 + (jax.ShapeDtypeStruct((SUB, width), f32),),
        in_specs=[vmem] * 5,
        out_specs=(vmem,) * 5,
        scratch_shapes=[
            pltpu.VMEM((2, rows + 4, layers + 2 * SUB, width), f32),
            pltpu.VMEM((2, layers, LANES), f32),
            pltpu.VMEM((2, layers, LANES), f32),
            pltpu.VMEM((2, layers, LANES), f32),
            pltpu.VMEM((2, chunks, 1, LANES), f32),
            pltpu.VMEM((2, chunks, 4, 1, LANES), f32),
            pltpu.VMEM((ITERS + 1, 2, layers, width), f32),
            pltpu.VMEM((ITERS + 2, rows, layers, width), f32),
            pltpu.VMEM((rows, layers, width), f32),
            pltpu.VMEM((rows, layers, width), f32),
            pltpu.VMEM((rows, layers, width), f32),
            pltpu.VMEM((2, rows, width), f32),
            pltpu.VMEM((2, rows, width), f32),
            pltpu.VMEM((2 * ITERS + 2, SUB, LANES), f32),
            pltpu.VMEM((nx * ny, 1, LANES), f32),
            pltpu.VMEM((nx * ny, 1, LANES), f32),
            dma((2, chunks, 8)),
            dma((2, chunks, 8)),
            dma((2,)),
            dma((4, 2, chunks)),
            dma((nx * ny - 1,)),
            dma((nx * ny - 1,)),
            dma((nx * ny - 1,)),
            dma((nx * ny - 1,)),
        ],
        compiler_params=pltpu.CompilerParams(
            collective_id=0, has_side_effects=True, vmem_limit_bytes=40 * 1024 * 1024
        ),
        name="krylov",
    )(forcing[0], turned(conduct), turned(diag_add), ice_mask, grounded)
    step = out_s[:1]
    solved, residual = out_x + step * out_p, out_r - step * out_q
    return tuple(o[None] for o in (solved, residual))


def solution(mesh):
    spec = P("group", None, "gx", "gy")
    flat = P("gx", "gy")
    return jax.shard_map(
        functools.partial(on_device, mesh.shape["gx"], mesh.shape["gy"]),
        mesh=mesh,
        in_specs=(spec, spec, spec, flat, flat),
        out_specs=(spec, spec),
        check_vma=False,
    )
```

```python
import functools

import jax
import jax.numpy as jnp
from jax import lax
from jax.experimental import pallas as pl
from jax.experimental.pallas import tpu as pltpu
from jax.sharding import PartitionSpec as P

ITERS = 6
far_weight = 0.25
cross_weight = 0.5
vertical_weight = 4.0
friction_gain = 8.0
SUB = 8
LANES = 128
CHUNK_TILES = (2, 1)


def coefficients(moments):
    def gram(j, k):
        return 0.5 * (moments[j + k] + moments[abs(j - k)])

    table = {
        (j, k): gram(j, k)
        for j in range(ITERS + 1)
        for k in range(j, ITERS + 1)
        if j + k < len(moments)
    }

    def form(a, b):
        terms = []
        for j in range(len(a)):
            row = None
            for k in range(len(b)):
                term = table[min(j, k), max(j, k)] * b[k]
                row = term if row is None else row + term
            terms.append(a[j] * row)
        return functools.reduce(lambda s, t: s + t, terms)

    def shift(e):
        out = [jnp.zeros_like(e[0]) for _ in range(len(e) + 1)]
        for k, value in enumerate(e):
            if k == 0:
                out[1] = out[1] + value
            else:
                out[k + 1] = out[k + 1] + 0.5 * value
                out[k - 1] = out[k - 1] + 0.5 * value
        return out

    left = [jnp.ones_like(moments[0])]
    direction = list(left)
    iterate = []
    norm_now = form(left, left)
    for iteration in range(ITERS):
        moved = shift(direction)
        applied = [
            (direction[k] - moved[k]) if k < len(direction) else -moved[k]
            for k in range(len(moved))
        ]
        if iteration + 1 == ITERS:
            table[iteration, ITERS] = 0.5 * moments[1]
            slope = 0.5 * direction[-1] * applied[-1]
            return iterate, left, direction, applied, norm_now, form(direction, applied), slope
        step = norm_now / form(direction, applied)
        iterate = [
            (iterate[k] if k < len(iterate) else 0.0) + step * direction[k]
            for k in range(len(direction))
        ]
        left = [
            (left[k] - step * applied[k]) if k < len(left) else -step * applied[k]
            for k in range(len(applied))
        ]
        norm_next = form(left, left)
        ratio = norm_next / norm_now
        direction = [
            left[k] + (ratio * direction[k] if k < len(direction) else 0.0)
            for k in range(len(left))
        ]
        norm_now = norm_next


def kernel(
    sizes,
    force,
    conduct,
    extra,
    ice,
    grounded,
    out_x,
    out_p,
    out_r,
    out_q,
    out_s,
    field,
    pack,
    rim_right,
    rim_left,
    corner,
    cornered,
    held,
    basis,
    coupling,
    scaled,
    diagonal,
    share,
    shared,
    partial,
    sum_early,
    sum_all,
    send_sem,
    recv_sem,
    share_sem,
    detour_sem,
    se_send,
    se_recv,
    sa_send,
    sa_recv,
):
    nx, ny = sizes
    rows, layers, width = conduct.shape
    tiles = layers // SUB
    chunks = send_sem.shape[1]
    per = tiles // chunks
    deep = per * SUB
    group = 2 if 8 * deep <= LANES else 1
    gg, gx, gy = lax.axis_index("group"), lax.axis_index("gx"), lax.axis_index("gy")
    is_ice = gg == 0

    def there(dx, dy):
        ok = None
        for d, g, n in ((dx, gx, nx), (dy, gy, ny)):
            if d != 0:
                one = (g + d >= 0) & (g + d < n)
                ok = one if ok is None else ok & one
        return ok

    def at(dx, dy):
        return (gg, gx + dx, gy + dy)

    two = 2 * rows
    sides = ((-1, 0), (1, 0), (0, -1), (0, 1), (-1, -1), (1, -1), (-1, 1), (1, 1))

    def copy_of(i, p, c, span=2):
        dx, dy = sides[i]
        inner = pl.ds(pl.multiple_of(c * deep + SUB, SUB), deep)
        flat = pl.ds(pl.multiple_of(c * deep, SUB), deep)
        if i == 0:
            source = field.at[p, 2 : 2 + span, inner]
            target = field.at[p, rows + 2 : rows + 2 + span, inner]
        elif i == 1:
            source = field.at[p, rows : rows + span, inner]
            target = field.at[p, 0:span, inner]
        elif i == 2:
            source, target = pack.at[p, flat], rim_right.at[p, flat]
        elif i == 3:
            source, target = pack.at[p, flat], rim_left.at[p, flat]
        else:
            source, target = corner.at[p, c // group], cornered.at[p, c // group, i - 4]
        return pltpu.make_async_remote_copy(
            src_ref=source,
            dst_ref=target,
            send_sem=send_sem.at[p, c if i < 4 else c // group * group, i],
            recv_sem=recv_sem.at[p, c if i < 4 else c // group * group, i],
            device_id=at(dx, dy),
            device_id_type=pl.DeviceIdType.MESH,
        )

    detours = ((1, 3, 2, rows, 0), (2, 0, 1, 2, rows + 2)) if nx == 4 else ()
    relayed = gg == 1
    lag = min(3, chunks - 1)

    def each(toward, act, chosen=range(8)):
        for i in chosen:
            dx, dy = sides[i]
            ok = there(toward * dx, toward * dy)
            if i < 2 and detours:
                split = gx == ((2 - i) if toward > 0 else (1 + i))

                ok = ok & jnp.logical_not(split & relayed)

            @pl.when(ok)
            def _():
                act(i, 2)

    def away(path, p, c, slot):
        origin, relay, _, row, _ = path
        return pltpu.make_async_remote_copy(
            src_ref=field.at[p, row : row + 2, pl.ds(pl.multiple_of(c * deep + SUB, SUB), deep)],
            dst_ref=held.at[slot, :, pl.ds(pl.multiple_of(c * deep, SUB), deep)],
            send_sem=detour_sem.at[0, p, c],
            recv_sem=detour_sem.at[1, p, c],
            device_id=(gg, relay, gy),
            device_id_type=pl.DeviceIdType.MESH,
        )

    def onward(path, p, c, slot):
        _, _, end, _, row = path
        return pltpu.make_async_remote_copy(
            src_ref=held.at[slot, :, pl.ds(pl.multiple_of(c * deep, SUB), deep)],
            dst_ref=field.at[p, row : row + 2, pl.ds(pl.multiple_of(c * deep + SUB, SUB), deep)],
            send_sem=detour_sem.at[2, p, c],
            recv_sem=detour_sem.at[3, p, c],
            device_id=(gg, end, gy),
            device_id_type=pl.DeviceIdType.MESH,
        )

    def forward(message):
        slot = message // chunks
        c = message % chunks
        p = slot % 2
        for path in detours:
            @pl.when((gx == path[1]) & relayed)
            def _():
                @pl.when(slot >= 2)
                def _():
                    onward(path, p, c, slot).wait_send()

                away(path, p, c, slot).wait_recv()
                onward(path, p, c, slot).start()

    def first_of(c):
        return lax.rem(c, group) == 0

    def last_of(c):
        return (lax.rem(c, group) == group - 1) | (c == chunks - 1)

    def start_rows(p, c, slot):
        for path in detours:
            @pl.when((gx == path[0]) & relayed)
            def _():
                away(path, p, c, slot).start()
        for order in ((1, 0), (0, 1)):
            @pl.when((gx == 2) if order == (0, 1) else (gx != 2))
            def _():
                each(1, lambda i, span: copy_of(i, p, c, span).start(), order)

        @pl.when(last_of(c))
        def _():
            each(1, lambda i, span: copy_of(i, p, c, span).start(), range(4, 8))

    def start_rest(p, c):
        each(1, lambda i, span: copy_of(i, p, c, span).start(), range(2, 4))

    def start(p, c, slot):
        start_rows(p, c, slot)
        start_rest(p, c)

    def finish_recv(p, c):
        for path in detours:
            @pl.when((gx == path[2]) & relayed)
            def _():
                onward(path, p, c, 0).wait_recv()
        each(-1, lambda i, span: copy_of(i, p, c, span).wait_recv(), range(4))

        @pl.when(first_of(c))
        def _():
            each(-1, lambda i, span: copy_of(i, p, c, span).wait_recv(), range(4, 8))

    def finish_send(p, c):
        for path in detours:
            @pl.when((gx == path[0]) & relayed)
            def _():
                away(path, p, c, 0).wait_send()
        each(1, lambda i, span: copy_of(i, p, c, span).wait_send(), range(4))

        @pl.when(first_of(c))
        def _():
            each(1, lambda i, span: copy_of(i, p, c, span).wait_send(), range(4, 8))

    barrier = pltpu.get_barrier_semaphore()

    def peers_all():
        me = gx * ny + gy
        out = []
        for o in range(1, nx * ny):
            peer = lax.rem(me + o, nx * ny)
            out.append((gg, peer // ny, lax.rem(peer, ny)))
        return out

    def greet(device):
        pl.semaphore_signal(
            barrier, inc=1, device_id=device, device_id_type=pl.DeviceIdType.MESH
        )

    greet((1 - gg, gx, gy))
    if max(nx, ny) < ITERS:
        met = jnp.int32(1)
        for dx, dy in sides:
            @pl.when(there(dx, dy))
            def _():
                greet(at(dx, dy))
            met = met + jnp.where(there(dx, dy), 1, 0).astype(jnp.int32)
        for origin, relay, end, _, _ in detours:
            for one, other in ((origin, relay), (relay, end)):
                for here, peer in ((one, other), (other, one)):
                    if abs(here - peer) > 1:
                        @pl.when(gx == here)
                        def _():
                            greet((gg, peer, gy))
                        met = met + jnp.where(gx == here, 1, 0).astype(jnp.int32)
    else:
        for device in peers_all():
            greet(device)
        met = jnp.int32(nx * ny)

    for p in range(2):
        for r, d in ((0, -1), (rows + 2, 1)):
            @pl.when(jnp.logical_not(there(d, 0)))
            def _():
                field[p, r : r + 2] = jnp.zeros((2, layers + 2 * SUB, width), jnp.float32)
        for r in range(2, rows + 2):
            for s in (0, SUB + layers):
                field[p, r, s : s + SUB] = jnp.zeros((SUB, width), jnp.float32)
        for ref, d in ((rim_left, -1), (rim_right, 1)):
            @pl.when(jnp.logical_not(there(0, d)))
            def _():
                ref[p] = jnp.zeros(ref.shape[1:], jnp.float32)
        for i in range(4):
            @pl.when(jnp.logical_not(there(-sides[4 + i][0], -sides[4 + i][1])))
            def _():
                for c in range(cornered.shape[1]):
                    cornered[p, c, i] = jnp.zeros((1, LANES), jnp.float32)

    lane = lax.broadcasted_iota(jnp.int32, (SUB, LANES), 1)
    sub = lax.broadcasted_iota(jnp.int32, (SUB, width), 0)

    tile_row = lax.broadcasted_iota(jnp.int32, (SUB, LANES), 0)

    def spot(i, t):
        return lane == (i * per + t) * SUB + tile_row

    def pack_row(x, value, tile, t, corners):
        first, last = value[:, :LANES], value[:, width - LANES :]
        low = first if x == 0 else pltpu.roll(first, 2 * x, 1)
        high = pltpu.roll(last, (two + 2 * x - LANES + 2) % LANES, 1)
        tile = jnp.where((lane >= 2 * x) & (lane < 2 * x + 2), low, tile)
        tile = jnp.where((lane >= two + 2 * x) & (lane < two + 2 * x + 2), high, tile)
        for i, (at_x, y) in enumerate(
            ((0, 0), (rows - 1, 0), (0, width - 1), (rows - 1, width - 1))
        ):
            if x == at_x:
                column = jnp.broadcast_to(value[:, y : y + 1], (SUB, LANES))
                corners = jnp.where(spot(i, t), column, corners)
        return tile, corners

    def put_corner(p, c, corners):
        value = jnp.sum(corners, axis=0, keepdims=True)

        @pl.when(first_of(c))
        def _():
            corner[p, c // group] = value

        if group > 1:

            @pl.when(jnp.logical_not(first_of(c)))
            def _():
                corner[p, c // group] = corner[p, c // group] + pltpu.roll(value, LANES // 2, 1)

    ice_cells = ice[...].astype(jnp.float32)
    ground_cells = grounded[...].astype(jnp.float32)
    ocean = jnp.where(is_ice, 0.0, 1.0).astype(jnp.float32)
    active = ice_cells * (1.0 - ocean * ground_cells)
    friction = (1.0 - ocean) * friction_gain * ground_cells * ice_cells

    def wide(array, x):
        return jnp.broadcast_to(array[x : x + 1, :], (SUB, width))

    blank = jnp.zeros((SUB, LANES), jnp.float32)
    zero = jnp.zeros((SUB, width), jnp.float32)

    def prepare(c):
        corners = blank
        for t in range(per):
            j = c * per + t
            ls = pl.ds(pl.multiple_of(j * SUB, SUB), SUB)
            tile = blank
            for x in range(rows):
                value = jnp.sqrt(conduct[x, ls, :]) * wide(active, x)
                coupling[x, ls, :] = value
                field[0, x + 2, pl.ds(pl.multiple_of(j * SUB + SUB, SUB), SUB), :] = value
                tile, corners = pack_row(x, value, tile, t, corners)
            pack[0, ls, :] = tile
        put_corner(0, c, corners)

    def first_pass(c, carry):
        start(0, c - 1, 0)

        @pl.when(c > lag)
        def _():
            forward(c - 1 - lag)

        prepare(c)
        return carry

    prepare(0)
    pl.semaphore_wait(barrier, met)
    lax.fori_loop(1, chunks, first_pass, 0)
    start(0, chunks - 1, 0)
    forward(chunks - 1 - lag)

    def gather(j, total):
        for t in range(SUB):
            total = total + force[j * SUB + t]
        return total

    total = lax.fori_loop(0, tiles, gather, jnp.zeros((rows, width), jnp.float32))
    share[0] = active * (total * (1.0 / layers))
    for x in range(rows):
        share[1, x : x + 1, :] = jnp.where(
            is_ice, coupling[x, 0:1, :], coupling[x, layers - 1 : layers, :]
        )

    to_partner = pltpu.make_async_remote_copy(
        src_ref=share,
        dst_ref=shared,
        send_sem=share_sem.at[0],
        recv_sem=share_sem.at[1],
        device_id=(1 - gg, gx, gy),
        device_id_type=pl.DeviceIdType.MESH,
    )
    to_partner.start()

    outer = tuple(x for x in range(rows) if x < 2 or x >= rows - 2)
    inner = tuple(x for x in range(rows) if x not in outer)

    def spread_block(p, c, t, xs):
        j = c * per + t
        here = pl.ds(pl.multiple_of(j * SUB + SUB, SUB), SUB)
        below = pl.ds(pl.multiple_of(j * SUB, SUB), SUB)
        above = pl.ds(pl.multiple_of(j * SUB + 2 * SUB, SUB), SUB)
        from_right, from_left = rim_right[p, below, :], rim_left[p, below, :]

        def column(i):
            row = jnp.broadcast_to(cornered[p, c // group, i], (SUB, LANES))
            if group > 1:
                row = jnp.where(first_of(c), row, pltpu.roll(row, LANES // 2, 1))
            return jnp.sum(jnp.where(spot(i, t), row, 0.0), axis=1, keepdims=True)

        def rim(x):
            right = from_right if x == 0 else pltpu.roll(from_right, LANES - 2 * x, 1)
            left = pltpu.roll(from_left, (LANES - 2 - two - 2 * x) % LANES, 1)
            return jnp.where(lane < LANES // 2, right, left)

        def line(x):
            if x == 0:
                edge = jnp.where(lane < LANES // 2, column(1), column(3))
            elif x == rows + 1:
                edge = jnp.where(lane < LANES // 2, column(0), column(2))
            else:
                edge = rim(x - 1)
            value = field[p, x + 1, here, :]
            return [value[:, l : l + LANES] for l in range(0, width, LANES)] + [edge]

        def shifted(tiles_in, by):
            count = len(tiles_in) - 1
            out = []
            for i in range(count):
                before, own, after = tiles_in[i - 1], tiles_in[i], tiles_in[i + 1]
                up = pltpu.roll(jnp.where(lane >= LANES - by, before, own), by, 1)
                down = pltpu.roll(jnp.where(lane < by, after, own), LANES - by, 1)
                out.append(up + down)
            return jnp.concatenate(out, axis=1)

        e = {}
        for x in xs:
            for i in range(x, x + 3):
                if i not in e:
                    e[i] = line(i)
            beside = [a + b for a, b in zip(e[x], e[x + 2])]
            h = [a + cross_weight * b for a, b in zip(e[x + 1], beside)]
            mine = field[p, x + 2, here, :]
            up = pltpu.roll(jnp.where(sub == 0, field[p, x + 2, above, :], mine), SUB - 1, 0)
            down = pltpu.roll(jnp.where(sub == SUB - 1, field[p, x + 2, below, :], mine), 1, 0)
            yield (
                shifted(h, 1)
                + jnp.concatenate(beside[:-1], axis=1)
                + far_weight
                * (shifted(e[x + 1], 2) + (field[p, x, here, :] + field[p, x + 4, here, :]))
                + vertical_weight * (up + down)
            )

    def fold(value):
        return functools.reduce(
            lambda s, t: s + t, [value[:, c : c + LANES] for c in range(0, width, LANES)]
        )

    to_partner.wait_recv()
    term = active * (shared[1] * shared[0])

    edge = jnp.where(is_ice, 0, layers - 1).astype(jnp.int32)

    def zeroth(c, acc):
        forward(chunks + c - lag)
        finish_recv(0, c)
        corners, packed = blank, [blank] * per
        for xs in (outer, inner):
            for t in range(per):
                j = c * per + t
                ls = pl.ds(pl.multiple_of(j * SUB, SUB), SUB)
                layer = sub + j * SUB
                at_edge = layer == edge
                at_bottom = layer == 0
                for x, around in zip(xs, list(spread_block(0, c, t, xs))):
                    own = coupling[x, ls, :]
                    diag = (
                        extra[x, ls, :]
                        + jnp.where(at_bottom, wide(friction, x), 0.0)
                        + own * around
                    )
                    inverse = 1.0 / diag
                    source = wide(active, x) * force[ls, x, :] + jnp.where(
                        at_edge, wide(term, x), 0.0
                    )
                    vector = inverse * source
                    diagonal[x, ls, :] = diag
                    scaled[x, ls, :] = inverse * own
                    basis[0, x, ls, :] = zero
                    basis[1, x, ls, :] = vector
                    value = own * vector
                    after = pl.ds(pl.multiple_of(j * SUB + SUB, SUB), SUB)
                    field[1, x + 2, after, :] = value
                    packed[t], corners = pack_row(x, value, packed[t], t, corners)
                    acc = acc + source * vector
                if xs is inner:
                    pack[1, ls, :] = packed[t]
            if xs is outer:
                put_corner(1, c, corners)
                start_rows(1, c, 1)
        start_rest(1, c)
        return acc

    partial[0] = fold(lax.fori_loop(0, chunks, zeroth, zero))
    partial[1] = blank
    to_partner.wait_send()

    lane_row = lax.broadcasted_iota(jnp.int32, (1, LANES), 1)

    def copies(slots, me, devices, sends, recvs):
        return [
            pltpu.make_async_remote_copy(
                src_ref=slots.at[me],
                dst_ref=slots.at[me],
                send_sem=sends.at[o],
                recv_sem=recvs.at[o],
                device_id=device,
                device_id_type=pl.DeviceIdType.MESH,
            )
            for o, device in enumerate(devices)
        ]

    def row_of(slots):
        return functools.reduce(lambda s, t: s + t, [slots[o] for o in range(slots.shape[0])])

    def copies_early():
        return copies(sum_early, gx * ny + gy, peers_all(), se_send, se_recv)

    def early_start():
        row = jnp.zeros((1, LANES), jnp.float32)
        for m in range(2 * ITERS):
            value = jnp.sum(partial[m], axis=0, keepdims=True)
            value = jnp.sum(value, axis=1, keepdims=True)
            row = jnp.where(lane_row == m, jnp.broadcast_to(value, (1, LANES)), row)
        sum_early[gx * ny + gy] = row
        for copy in copies_early():
            copy.start()

    def early_finish():
        for copy in copies_early():
            copy.wait_recv()
        for copy in copies_early():
            copy.wait_send()

    def step(k, carry):
        p = lax.rem(k, 2)
        q = 1 - p
        gain = jnp.where(k == 1, 1.0, 2.0).astype(jnp.float32)

        def block(c, accs):
            own_acc, cross_acc = accs
            message = (k + 1) * chunks + c - lag

            @pl.when(message < (ITERS + 1) * chunks)
            def _():
                forward(message)

            finish_recv(p, c)
            finish_send(q, c)
            corners, packed = blank, [blank] * per
            for xs in (outer, inner):
                for t in range(per):
                    j = c * per + t
                    ls = pl.ds(pl.multiple_of(j * SUB, SUB), SUB)
                    vectors, values = [], []
                    for x, around in zip(xs, list(spread_block(p, c, t, xs))):
                        vector = gain * (scaled[x, ls, :] * around) - basis[k - 1, x, ls, :]
                        weighted = diagonal[x, ls, :] * vector
                        value = coupling[x, ls, :] * vector
                        own_acc = own_acc + weighted * vector
                        cross_acc = cross_acc + weighted * basis[k, x, ls, :]
                        packed[t], corners = pack_row(x, value, packed[t], t, corners)
                        vectors.append(vector)
                        values.append(value)
                    after = pl.ds(pl.multiple_of(j * SUB + SUB, SUB), SUB)
                    for x, vector, value in zip(xs, vectors, values):
                        basis[k + 1, x, ls, :] = vector
                        field[q, x + 2, after, :] = value
                    if xs is inner:
                        pack[q, ls, :] = packed[t]
                if xs is outer:
                    put_corner(q, c, corners)

                    @pl.when(k < ITERS)
                    def _():
                        start_rows(q, c, k + 1)

            @pl.when(k < ITERS)
            def _():
                start_rest(q, c)

            return own_acc, cross_acc

        own_acc, cross_acc = lax.fori_loop(0, chunks, block, (zero, zero))
        partial[2 * k] = fold(own_acc)
        partial[2 * k + 1] = fold(cross_acc)

        @pl.when(k == ITERS - 1)
        def _():
            early_start()

        return carry

    lax.fori_loop(1, ITERS + 1, step, 0)
    sum_all[gx * ny + gy] = jnp.sum(partial[2 * ITERS + 1], axis=0, keepdims=True)
    to_all = copies(sum_all, gx * ny + gy, peers_all(), sa_send, sa_recv)
    for copy in to_all:
        copy.start()

    def settle(c, carry):
        finish_send(ITERS % 2, c)
        for path in detours:
            @pl.when((gx == path[1]) & relayed)
            def _():
                for p in range(2):
                    onward(path, p, c, 0).wait_send()
        return carry

    lax.fori_loop(0, chunks, settle, 0)

    early_finish()
    total = row_of(sum_early)
    dots = [jnp.broadcast_to(total[:, m : m + 1], (SUB, LANES)) for m in range(2 * ITERS)]
    moments = [dots[0], dots[3]]
    for k in range(1, ITERS):
        if k > 1:
            moments.append(2.0 * dots[2 * k + 1] - moments[1])
        moments.append(2.0 * dots[2 * k] - moments[0])
    *lists, norm, fixed, slope = coefficients(moments)

    def widen(value):
        return jnp.concatenate([value] * (width // LANES), axis=1)

    iterate, left, direction, applied = [[widen(v) for v in values] for values in lists]

    def combined(values, us):
        return functools.reduce(lambda s, t: s + t, [a * u for a, u in zip(values, us)])

    def last(j, carry):
        ls = pl.ds(pl.multiple_of(j * SUB, SUB), SUB)
        for x in range(rows):
            us = [basis[k + 1, x, ls, :] for k in range(ITERS + 1)]
            diag = diagonal[x, ls, :]
            out_x[ls, x, :] = combined(iterate, us)
            out_p[ls, x, :] = combined(direction, us)
            out_r[ls, x, :] = diag * combined(left, us)
            out_q[ls, x, :] = diag * combined(applied, us)
        return carry

    lax.fori_loop(0, tiles, last, 0)

    for copy in to_all:
        copy.wait_recv()
    cross = jnp.sum(row_of(sum_all), axis=1, keepdims=True)
    cross = jnp.broadcast_to(cross, (SUB, LANES))
    out_s[...] = widen(norm / (fixed + slope * (2.0 * cross - moments[1])))
    for copy in to_all:
        copy.wait_send()


def on_device(nx, ny, forcing, conduct, diag_add, ice_mask, grounded):
    def turned(a):
        return jnp.transpose(a[0].astype(jnp.float32), (1, 0, 2))

    _, layers, rows, width = forcing.shape
    tiles = layers // SUB
    chunks = tiles // next(t for t in CHUNK_TILES if tiles % t == 0)
    pairs = 2 if 8 * (layers // chunks) <= LANES else 1
    rows_of_corners = -(-chunks // pairs)
    f32 = jnp.float32
    block = jax.ShapeDtypeStruct((rows, layers, width), f32)
    vmem = pl.BlockSpec(memory_space=pltpu.VMEM)
    dma = pltpu.SemaphoreType.DMA
    out_x, out_p, out_r, out_q, out_s = pl.pallas_call(
        functools.partial(kernel, (nx, ny)),
        out_shape=(jax.ShapeDtypeStruct((layers, rows, width), f32),) * 4 + (jax.ShapeDtypeStruct((SUB, width), f32),),
        in_specs=[vmem] * 5,
        out_specs=(vmem,) * 5,
        scratch_shapes=[
            pltpu.VMEM((2, rows + 4, layers + 2 * SUB, width), f32),
            pltpu.VMEM((2, layers, LANES), f32),
            pltpu.VMEM((2, layers, LANES), f32),
            pltpu.VMEM((2, layers, LANES), f32),
            pltpu.VMEM((2, rows_of_corners, 1, LANES), f32),
            pltpu.VMEM((2, rows_of_corners, 4, 1, LANES), f32),
            pltpu.VMEM((ITERS + 1, 2, layers, width), f32),
            pltpu.VMEM((ITERS + 2, rows, layers, width), f32),
            pltpu.VMEM((rows, layers, width), f32),
            pltpu.VMEM((rows, layers, width), f32),
            pltpu.VMEM((rows, layers, width), f32),
            pltpu.VMEM((2, rows, width), f32),
            pltpu.VMEM((2, rows, width), f32),
            pltpu.VMEM((2 * ITERS + 2, SUB, LANES), f32),
            pltpu.VMEM((nx * ny, 1, LANES), f32),
            pltpu.VMEM((nx * ny, 1, LANES), f32),
            dma((2, chunks, 8)),
            dma((2, chunks, 8)),
            dma((2,)),
            dma((4, 2, chunks)),
            dma((nx * ny - 1,)),
            dma((nx * ny - 1,)),
            dma((nx * ny - 1,)),
            dma((nx * ny - 1,)),
        ],
        compiler_params=pltpu.CompilerParams(
            collective_id=0, has_side_effects=True, vmem_limit_bytes=40 * 1024 * 1024
        ),
        name="krylov",
    )(forcing[0], turned(conduct), turned(diag_add), ice_mask, grounded)
    step = out_s[:1]
    solved, residual = out_x + step * out_p, out_r - step * out_q
    return tuple(o[None] for o in (solved, residual))


def solution(mesh):
    spec = P("group", None, "gx", "gy")
    flat = P("gx", "gy")
    return jax.shard_map(
        functools.partial(on_device, mesh.shape["gx"], mesh.shape["gy"]),
        mesh=mesh,
        in_specs=(spec, spec, spec, flat, flat),
        out_specs=(spec, spec),
        check_vma=False,
    )
```

```python
import functools

import jax
import jax.numpy as jnp
from jax import lax
from jax.experimental import pallas as pl
from jax.experimental.pallas import tpu as pltpu
from jax.sharding import PartitionSpec as P

ITERS = 6
far_weight = 0.25
cross_weight = 0.5
vertical_weight = 4.0
friction_gain = 8.0
SUB = 8
LANES = 128
CHUNK_TILES = (2, 1)


def coefficients(moments):
    def gram(j, k):
        return 0.5 * (moments[j + k] + moments[abs(j - k)])

    table = {
        (j, k): gram(j, k)
        for j in range(ITERS + 1)
        for k in range(j, ITERS + 1)
        if j + k < len(moments)
    }

    def form(a, b):
        terms = []
        for j in range(len(a)):
            row = None
            for k in range(len(b)):
                term = table[min(j, k), max(j, k)] * b[k]
                row = term if row is None else row + term
            terms.append(a[j] * row)
        return functools.reduce(lambda s, t: s + t, terms)

    def shift(e):
        out = [jnp.zeros_like(e[0]) for _ in range(len(e) + 1)]
        for k, value in enumerate(e):
            if k == 0:
                out[1] = out[1] + value
            else:
                out[k + 1] = out[k + 1] + 0.5 * value
                out[k - 1] = out[k - 1] + 0.5 * value
        return out

    left = [jnp.ones_like(moments[0])]
    direction = list(left)
    iterate = []
    norm_now = form(left, left)
    for iteration in range(ITERS):
        moved = shift(direction)
        applied = [
            (direction[k] - moved[k]) if k < len(direction) else -moved[k]
            for k in range(len(moved))
        ]
        if iteration + 1 == ITERS:
            table[iteration, ITERS] = 0.5 * moments[1]
            slope = 0.5 * direction[-1] * applied[-1]
            return iterate, left, direction, applied, norm_now, form(direction, applied), slope
        step = norm_now / form(direction, applied)
        iterate = [
            (iterate[k] if k < len(iterate) else 0.0) + step * direction[k]
            for k in range(len(direction))
        ]
        left = [
            (left[k] - step * applied[k]) if k < len(left) else -step * applied[k]
            for k in range(len(applied))
        ]
        norm_next = form(left, left)
        ratio = norm_next / norm_now
        direction = [
            left[k] + (ratio * direction[k] if k < len(direction) else 0.0)
            for k in range(len(left))
        ]
        norm_now = norm_next


def kernel(
    sizes,
    force,
    conduct,
    extra_half,
    active_cells,
    friction_cells,
    out_x,
    out_p,
    out_r,
    out_q,
    out_s,
    field,
    pack,
    rim_right,
    rim_left,
    corner,
    cornered,
    held,
    basis,
    coupling,
    scaled,
    diagonal,
    share,
    shared,
    partial,
    sum_early,
    sum_all,
    send_sem,
    recv_sem,
    share_sem,
    detour_sem,
    se_send,
    se_recv,
    sa_send,
    sa_recv,
    extra,
):
    nx, ny = sizes
    layers, rows, width = conduct.shape
    tiles = layers // SUB
    chunks = send_sem.shape[1]
    per = tiles // chunks
    deep = per * SUB
    group = 2 if 8 * deep <= LANES else 1
    gg, gx, gy = lax.axis_index("group"), lax.axis_index("gx"), lax.axis_index("gy")
    is_ice = gg == 0

    def there(dx, dy):
        ok = None
        for d, g, n in ((dx, gx, nx), (dy, gy, ny)):
            if d != 0:
                one = (g + d >= 0) & (g + d < n)
                ok = one if ok is None else ok & one
        return ok

    def at(dx, dy):
        return (gg, gx + dx, gy + dy)

    two = 2 * rows
    sides = ((-1, 0), (1, 0), (0, -1), (0, 1), (-1, -1), (1, -1), (-1, 1), (1, 1))

    def copy_of(i, p, c, span=2):
        dx, dy = sides[i]
        inner = pl.ds(pl.multiple_of(c * deep + SUB, SUB), deep)
        flat = pl.ds(pl.multiple_of(c * deep, SUB), deep)
        if i == 0:
            source = field.at[p, 2 : 2 + span, inner]
            target = field.at[p, rows + 2 : rows + 2 + span, inner]
        elif i == 1:
            source = field.at[p, rows : rows + span, inner]
            target = field.at[p, 0:span, inner]
        elif i == 2:
            source, target = pack.at[p, flat], rim_right.at[p, flat]
        elif i == 3:
            source, target = pack.at[p, flat], rim_left.at[p, flat]
        else:
            source, target = corner.at[p, c // group], cornered.at[p, c // group, i - 4]
        return pltpu.make_async_remote_copy(
            src_ref=source,
            dst_ref=target,
            send_sem=send_sem.at[p, c if i < 4 else c // group * group, i],
            recv_sem=recv_sem.at[p, c if i < 4 else c // group * group, i],
            device_id=at(dx, dy),
            device_id_type=pl.DeviceIdType.MESH,
        )

    detours = ((1, 3, 2, rows, 0), (2, 0, 1, 2, rows + 2)) if nx == 4 else ()
    relayed = gg == 1
    lag = min(3, chunks - 1)

    def each(toward, act, chosen=range(8)):
        for i in chosen:
            dx, dy = sides[i]
            ok = there(toward * dx, toward * dy)
            if i < 2 and detours:
                split = gx == ((2 - i) if toward > 0 else (1 + i))

                ok = ok & jnp.logical_not(split & relayed)

            @pl.when(ok)
            def _():
                act(i, 2)

    def away(path, p, c, slot):
        origin, relay, _, row, _ = path
        return pltpu.make_async_remote_copy(
            src_ref=field.at[p, row : row + 2, pl.ds(pl.multiple_of(c * deep + SUB, SUB), deep)],
            dst_ref=held.at[slot, :, pl.ds(pl.multiple_of(c * deep, SUB), deep)],
            send_sem=detour_sem.at[0, p, c],
            recv_sem=detour_sem.at[1, p, c],
            device_id=(gg, relay, gy),
            device_id_type=pl.DeviceIdType.MESH,
        )

    def onward(path, p, c, slot):
        _, _, end, _, row = path
        return pltpu.make_async_remote_copy(
            src_ref=held.at[slot, :, pl.ds(pl.multiple_of(c * deep, SUB), deep)],
            dst_ref=field.at[p, row : row + 2, pl.ds(pl.multiple_of(c * deep + SUB, SUB), deep)],
            send_sem=detour_sem.at[2, p, c],
            recv_sem=detour_sem.at[3, p, c],
            device_id=(gg, end, gy),
            device_id_type=pl.DeviceIdType.MESH,
        )

    def forward(message):
        slot = message // chunks
        c = message % chunks
        p = slot % 2
        for path in detours:
            @pl.when((gx == path[1]) & relayed)
            def _():
                @pl.when(slot >= 2)
                def _():
                    onward(path, p, c, slot).wait_send()

                away(path, p, c, slot).wait_recv()
                onward(path, p, c, slot).start()

    def first_of(c):
        return lax.rem(c, group) == 0

    def last_of(c):
        return (lax.rem(c, group) == group - 1) | (c == chunks - 1)

    def start_rows(p, c, slot):
        for path in detours:
            @pl.when((gx == path[0]) & relayed)
            def _():
                away(path, p, c, slot).start()
        for order in ((1, 0), (0, 1)):
            @pl.when((gx == 2) if order == (0, 1) else (gx != 2))
            def _():
                each(1, lambda i, span: copy_of(i, p, c, span).start(), order)

        @pl.when(last_of(c))
        def _():
            each(1, lambda i, span: copy_of(i, p, c, span).start(), range(4, 8))

    def start_rest(p, c):
        each(1, lambda i, span: copy_of(i, p, c, span).start(), range(2, 4))

    def start(p, c, slot):
        start_rows(p, c, slot)
        start_rest(p, c)

    def finish_rows(p, c):
        for path in detours:
            @pl.when((gx == path[2]) & relayed)
            def _():
                onward(path, p, c, 0).wait_recv()
        each(-1, lambda i, span: copy_of(i, p, c, span).wait_recv(), range(2))

        @pl.when(first_of(c))
        def _():
            each(-1, lambda i, span: copy_of(i, p, c, span).wait_recv(), range(4, 8))

    def finish_columns(p, c):
        each(-1, lambda i, span: copy_of(i, p, c, span).wait_recv(), range(2, 4))

    def finish_recv(p, c):
        finish_columns(p, c)
        finish_rows(p, c)

    def finish_send(p, c):
        for path in detours:
            @pl.when((gx == path[0]) & relayed)
            def _():
                away(path, p, c, 0).wait_send()
        each(1, lambda i, span: copy_of(i, p, c, span).wait_send(), range(4))

        @pl.when(first_of(c))
        def _():
            each(1, lambda i, span: copy_of(i, p, c, span).wait_send(), range(4, 8))

    barrier = pltpu.get_barrier_semaphore()

    def peers_all():
        me = gx * ny + gy
        out = []
        for o in range(1, nx * ny):
            peer = lax.rem(me + o, nx * ny)
            out.append((gg, peer // ny, lax.rem(peer, ny)))
        return out

    def greet(device):
        pl.semaphore_signal(
            barrier, inc=1, device_id=device, device_id_type=pl.DeviceIdType.MESH
        )

    greet((1 - gg, gx, gy))
    if max(nx, ny) < ITERS:
        met = jnp.int32(1)
        for dx, dy in sides:
            @pl.when(there(dx, dy))
            def _():
                greet(at(dx, dy))
            met = met + jnp.where(there(dx, dy), 1, 0).astype(jnp.int32)
        for origin, relay, end, _, _ in detours:
            for one, other in ((origin, relay), (relay, end)):
                for here, peer in ((one, other), (other, one)):
                    if abs(here - peer) > 1:
                        @pl.when(gx == here)
                        def _():
                            greet((gg, peer, gy))
                        met = met + jnp.where(gx == here, 1, 0).astype(jnp.int32)
    else:
        for device in peers_all():
            greet(device)
        met = jnp.int32(nx * ny)

    for p in range(2):
        for r, d in ((0, -1), (rows + 2, 1)):
            @pl.when(jnp.logical_not(there(d, 0)))
            def _():
                field[p, r : r + 2] = jnp.zeros((2, layers + 2 * SUB, width), jnp.float32)
        for r in range(2, rows + 2):
            for s in (0, SUB + layers):
                field[p, r, s : s + SUB] = jnp.zeros((SUB, width), jnp.float32)
        for ref, d in ((rim_left, -1), (rim_right, 1)):
            @pl.when(jnp.logical_not(there(0, d)))
            def _():
                ref[p] = jnp.zeros(ref.shape[1:], jnp.float32)
        for i in range(4):
            @pl.when(jnp.logical_not(there(-sides[4 + i][0], -sides[4 + i][1])))
            def _():
                for c in range(cornered.shape[1]):
                    cornered[p, c, i] = jnp.zeros((1, LANES), jnp.float32)

    lane = lax.broadcasted_iota(jnp.int32, (SUB, LANES), 1)
    sub = lax.broadcasted_iota(jnp.int32, (SUB, width), 0)

    tile_row = lax.broadcasted_iota(jnp.int32, (SUB, LANES), 0)

    def spot(i, t):
        return lane == (i * per + t) * SUB + tile_row

    def pack_row(x, value, tile, t, corners):
        first, last = value[:, :LANES], value[:, width - LANES :]
        low = first if x == 0 else pltpu.roll(first, 2 * x, 1)
        high = pltpu.roll(last, (two + 2 * x - LANES + 2) % LANES, 1)
        tile = jnp.where((lane >= 2 * x) & (lane < 2 * x + 2), low, tile)
        tile = jnp.where((lane >= two + 2 * x) & (lane < two + 2 * x + 2), high, tile)
        for i, (at_x, y) in enumerate(
            ((0, 0), (rows - 1, 0), (0, width - 1), (rows - 1, width - 1))
        ):
            if x == at_x:
                column = jnp.broadcast_to(value[:, y : y + 1], (SUB, LANES))
                corners = jnp.where(spot(i, t), column, corners)
        return tile, corners

    def put_corner(p, c, corners):
        value = jnp.sum(corners, axis=0, keepdims=True)

        @pl.when(first_of(c))
        def _():
            corner[p, c // group] = value

        if group > 1:

            @pl.when(jnp.logical_not(first_of(c)))
            def _():
                corner[p, c // group] = corner[p, c // group] + pltpu.roll(value, LANES // 2, 1)

    active, friction = active_cells[...], friction_cells[...]

    def wide(array, x):
        return jnp.broadcast_to(array[x : x + 1, :], (SUB, width))

    blank = jnp.zeros((SUB, LANES), jnp.float32)
    zero = jnp.zeros((SUB, width), jnp.float32)

    def prepare(c):
        corners = blank
        for t in range(per):
            j = c * per + t
            ls = pl.ds(pl.multiple_of(j * SUB, SUB), SUB)
            tile = blank
            for x in range(rows):
                value = jnp.sqrt(conduct[ls, x, :]) * wide(active, x)
                coupling[x, ls, :] = value
                field[0, x + 2, pl.ds(pl.multiple_of(j * SUB + SUB, SUB), SUB), :] = value
                tile, corners = pack_row(x, value, tile, t, corners)
            pack[0, ls, :] = tile
        put_corner(0, c, corners)

    def first_pass(c, carry):
        start(0, c - 1, 0)

        @pl.when(c > lag)
        def _():
            forward(c - 1 - lag)

        prepare(c)
        return carry

    prepare(0)
    pl.semaphore_wait(barrier, met)
    lax.fori_loop(1, chunks, first_pass, 0)
    start(0, chunks - 1, 0)
    forward(chunks - 1 - lag)

    def gather(j, total):
        for t in range(SUB):
            extra[j * SUB + t] = extra_half[j * SUB + t].astype(jnp.float32)
            total = total + force[j * SUB + t]
        return total

    total = lax.fori_loop(0, tiles, gather, jnp.zeros((rows, width), jnp.float32))
    share[0] = active * (total * (1.0 / layers))
    for x in range(rows):
        share[1, x : x + 1, :] = jnp.where(
            is_ice, coupling[x, 0:1, :], coupling[x, layers - 1 : layers, :]
        )

    to_partner = pltpu.make_async_remote_copy(
        src_ref=share,
        dst_ref=shared,
        send_sem=share_sem.at[0],
        recv_sem=share_sem.at[1],
        device_id=(1 - gg, gx, gy),
        device_id_type=pl.DeviceIdType.MESH,
    )
    to_partner.start()

    outer = tuple(x for x in range(rows) if x < 2 or x >= rows - 2)
    inner = tuple(x for x in range(rows) if x not in outer)

    def spread_block(p, c, t, xs):
        j = c * per + t
        here = pl.ds(pl.multiple_of(j * SUB + SUB, SUB), SUB)
        below = pl.ds(pl.multiple_of(j * SUB, SUB), SUB)
        above = pl.ds(pl.multiple_of(j * SUB + 2 * SUB, SUB), SUB)
        from_right, from_left = rim_right[p, below, :], rim_left[p, below, :]

        def column(i):
            row = jnp.broadcast_to(cornered[p, c // group, i], (SUB, LANES))
            if group > 1:
                row = jnp.where(first_of(c), row, pltpu.roll(row, LANES // 2, 1))
            return jnp.sum(jnp.where(spot(i, t), row, 0.0), axis=1, keepdims=True)

        def rim(x):
            right = from_right if x == 0 else pltpu.roll(from_right, LANES - 2 * x, 1)
            left = pltpu.roll(from_left, (LANES - 2 - two - 2 * x) % LANES, 1)
            return jnp.where(lane < LANES // 2, right, left)

        def line(x):
            if x == 0:
                edge = jnp.where(lane < LANES // 2, column(1), column(3))
            elif x == rows + 1:
                edge = jnp.where(lane < LANES // 2, column(0), column(2))
            else:
                edge = rim(x - 1)
            value = field[p, x + 1, here, :]
            return [value[:, l : l + LANES] for l in range(0, width, LANES)] + [edge]

        def shifted(tiles_in, by):
            count = len(tiles_in) - 1
            out = []
            for i in range(count):
                before, own, after = tiles_in[i - 1], tiles_in[i], tiles_in[i + 1]
                up = pltpu.roll(jnp.where(lane >= LANES - by, before, own), by, 1)
                down = pltpu.roll(jnp.where(lane < by, after, own), LANES - by, 1)
                out.append(up + down)
            return jnp.concatenate(out, axis=1)

        e = {}
        for x in xs:
            for i in range(x, x + 3):
                if i not in e:
                    e[i] = line(i)
            beside = [a + b for a, b in zip(e[x], e[x + 2])]
            h = [a + cross_weight * b for a, b in zip(e[x + 1], beside)]
            mine = field[p, x + 2, here, :]
            up = pltpu.roll(jnp.where(sub == 0, field[p, x + 2, above, :], mine), SUB - 1, 0)
            down = pltpu.roll(jnp.where(sub == SUB - 1, field[p, x + 2, below, :], mine), 1, 0)
            yield (
                shifted(h, 1)
                + jnp.concatenate(beside[:-1], axis=1)
                + far_weight
                * (shifted(e[x + 1], 2) + (field[p, x, here, :] + field[p, x + 4, here, :]))
                + vertical_weight * (up + down)
            )

    def fold(value):
        return functools.reduce(
            lambda s, t: s + t, [value[:, c : c + LANES] for c in range(0, width, LANES)]
        )

    to_partner.wait_recv()
    term = active * (shared[1] * shared[0])

    edge = jnp.where(is_ice, 0, layers - 1).astype(jnp.int32)

    def zeroth(c, acc):
        forward(chunks + c - lag)
        finish_recv(0, c)
        corners, packed = blank, [blank] * per
        for xs in (outer, inner):
            for t in range(per):
                j = c * per + t
                ls = pl.ds(pl.multiple_of(j * SUB, SUB), SUB)
                layer = sub + j * SUB
                at_edge = layer == edge
                at_bottom = layer == 0
                for x, around in zip(xs, list(spread_block(0, c, t, xs))):
                    own = coupling[x, ls, :]
                    diag = (
                        extra[ls, x, :]
                        + jnp.where(at_bottom, wide(friction, x), 0.0)
                        + own * around
                    )
                    inverse = 1.0 / diag
                    source = wide(active, x) * force[ls, x, :] + jnp.where(
                        at_edge, wide(term, x), 0.0
                    )
                    vector = inverse * source
                    diagonal[x, ls, :] = diag
                    scaled[x, ls, :] = inverse * own
                    basis[0, x, ls, :] = zero
                    basis[1, x, ls, :] = vector
                    value = own * vector
                    after = pl.ds(pl.multiple_of(j * SUB + SUB, SUB), SUB)
                    field[1, x + 2, after, :] = value
                    packed[t], corners = pack_row(x, value, packed[t], t, corners)
                    acc = acc + source * vector
                if xs is inner:
                    pack[1, ls, :] = packed[t]
            if xs is outer:
                put_corner(1, c, corners)
                start_rows(1, c, 1)
        start_rest(1, c)
        return acc

    partial[0] = fold(lax.fori_loop(0, chunks, zeroth, zero))
    partial[1] = blank
    to_partner.wait_send()

    lane_row = lax.broadcasted_iota(jnp.int32, (1, LANES), 1)

    def copies(slots, me, devices, sends, recvs):
        return [
            pltpu.make_async_remote_copy(
                src_ref=slots.at[me],
                dst_ref=slots.at[me],
                send_sem=sends.at[o],
                recv_sem=recvs.at[o],
                device_id=device,
                device_id_type=pl.DeviceIdType.MESH,
            )
            for o, device in enumerate(devices)
        ]

    def row_of(slots):
        return functools.reduce(lambda s, t: s + t, [slots[o] for o in range(slots.shape[0])])

    def copies_early():
        return copies(sum_early, gx * ny + gy, peers_all(), se_send, se_recv)

    def early_start():
        row = jnp.zeros((1, LANES), jnp.float32)
        for m in range(2 * ITERS):
            value = jnp.sum(partial[m], axis=0, keepdims=True)
            value = jnp.sum(value, axis=1, keepdims=True)
            row = jnp.where(lane_row == m, jnp.broadcast_to(value, (1, LANES)), row)
        sum_early[gx * ny + gy] = row
        for copy in copies_early():
            copy.start()

    def early_finish():
        for copy in copies_early():
            copy.wait_recv()
        for copy in copies_early():
            copy.wait_send()

    def step(k, carry):
        p = lax.rem(k, 2)
        q = 1 - p
        gain = jnp.where(k == 1, 1.0, 2.0).astype(jnp.float32)

        def block(c, accs):
            own_acc, cross_acc = accs
            forward((k + 1) * chunks + c - lag)
            finish_recv(p, c)
            finish_send(q, c)
            corners, packed = blank, [blank] * per
            for xs in (outer, inner):
                for t in range(per):
                    j = c * per + t
                    ls = pl.ds(pl.multiple_of(j * SUB, SUB), SUB)
                    vectors, values = [], []
                    for x, around in zip(xs, list(spread_block(p, c, t, xs))):
                        vector = gain * (scaled[x, ls, :] * around) - basis[k - 1, x, ls, :]
                        weighted = diagonal[x, ls, :] * vector
                        value = coupling[x, ls, :] * vector
                        own_acc = own_acc + weighted * vector
                        cross_acc = cross_acc + weighted * basis[k, x, ls, :]
                        packed[t], corners = pack_row(x, value, packed[t], t, corners)
                        vectors.append(vector)
                        values.append(value)
                    after = pl.ds(pl.multiple_of(j * SUB + SUB, SUB), SUB)
                    for x, vector, value in zip(xs, vectors, values):
                        basis[k + 1, x, ls, :] = vector
                        field[q, x + 2, after, :] = value
                    if xs is inner:
                        pack[q, ls, :] = packed[t]
                if xs is outer:
                    put_corner(q, c, corners)

                    start_rows(q, c, k + 1)

            start_rest(q, c)
            return own_acc, cross_acc

        own_acc, cross_acc = lax.fori_loop(0, chunks, block, (zero, zero))
        partial[2 * k] = fold(own_acc)
        partial[2 * k + 1] = fold(cross_acc)

        return carry

    lax.fori_loop(1, ITERS, step, 0)
    early_start()
    now = ITERS % 2

    def final_rows(c, acc, xs):
        for t in range(per):
            ls = pl.ds(pl.multiple_of((c * per + t) * SUB, SUB), SUB)
            for x, around in zip(xs, list(spread_block(now, c, t, xs))):
                vector = 2.0 * (scaled[x, ls, :] * around) - basis[ITERS - 1, x, ls, :]
                acc = acc + diagonal[x, ls, :] * vector * basis[ITERS, x, ls, :]
                basis[ITERS + 1, x, ls, :] = vector
        return acc

    def final_block(c, acc):
        @pl.when(c < lag)
        def _():
            forward((ITERS + 1) * chunks + c - lag)

        finish_columns(now, c)
        acc = final_rows(c, acc, inner)
        finish_rows(now, c)
        return final_rows(c, acc, outer)

    acc = fold(lax.fori_loop(0, chunks, final_block, zero))
    sum_all[gx * ny + gy] = jnp.sum(acc, axis=0, keepdims=True)
    to_all = copies(sum_all, gx * ny + gy, peers_all(), sa_send, sa_recv)
    for copy in to_all:
        copy.start()

    def settle(c, carry):
        finish_send(1 - now, c)
        finish_send(now, c)
        for path in detours:
            @pl.when((gx == path[1]) & relayed)
            def _():
                for p in range(2):
                    onward(path, p, c, 0).wait_send()
        return carry

    lax.fori_loop(0, chunks, settle, 0)

    early_finish()
    total = row_of(sum_early)
    dots = [jnp.broadcast_to(total[:, m : m + 1], (SUB, LANES)) for m in range(2 * ITERS)]
    moments = [dots[0], dots[3]]
    for k in range(1, ITERS):
        if k > 1:
            moments.append(2.0 * dots[2 * k + 1] - moments[1])
        moments.append(2.0 * dots[2 * k] - moments[0])
    *lists, norm, fixed, slope = coefficients(moments)

    def widen(value):
        return jnp.concatenate([value] * (width // LANES), axis=1)

    iterate, left, direction, applied = [[widen(v) for v in values] for values in lists]

    def combined(values, us):
        return functools.reduce(lambda s, t: s + t, [a * u for a, u in zip(values, us)])

    def last(j, carry):
        ls = pl.ds(pl.multiple_of(j * SUB, SUB), SUB)
        for x in range(rows):
            us = [basis[k + 1, x, ls, :] for k in range(ITERS + 1)]
            diag = diagonal[x, ls, :]
            out_x[ls, x, :] = combined(iterate, us)
            out_p[ls, x, :] = combined(direction, us)
            out_r[ls, x, :] = diag * combined(left, us)
            out_q[ls, x, :] = diag * combined(applied, us)
        return carry

    lax.fori_loop(0, tiles, last, 0)

    for copy in to_all:
        copy.wait_recv()
    cross = jnp.sum(row_of(sum_all), axis=1, keepdims=True)
    cross = jnp.broadcast_to(cross, (SUB, LANES))
    out_s[...] = widen(norm / (fixed + slope * (2.0 * cross - moments[1])))
    for copy in to_all:
        copy.wait_send()


def on_device(nx, ny, forcing, conduct, diag_add, ice_mask, grounded):
    wide_conduct = conduct[0].astype(jnp.float32)
    wide_conduct, ice_mask, grounded = lax.optimization_barrier(
        (wide_conduct, ice_mask, grounded)
    )
    ice_cells, ground_cells = ice_mask.astype(jnp.float32), grounded.astype(jnp.float32)
    ocean = jnp.where(lax.axis_index("group") == 0, 0.0, 1.0)
    active = ice_cells * (1.0 - ocean * ground_cells)
    friction = (1.0 - ocean) * friction_gain * ground_cells * ice_cells
    _, layers, rows, width = forcing.shape
    tiles = layers // SUB
    chunks = tiles // next(t for t in CHUNK_TILES if tiles % t == 0)
    pairs = 2 if 8 * (layers // chunks) <= LANES else 1
    rows_of_corners = -(-chunks // pairs)
    f32 = jnp.float32
    block = jax.ShapeDtypeStruct((rows, layers, width), f32)
    vmem = pl.BlockSpec(memory_space=pltpu.VMEM)
    dma = pltpu.SemaphoreType.DMA
    out_x, out_p, out_r, out_q, out_s = pl.pallas_call(
        functools.partial(kernel, (nx, ny)),
        out_shape=(jax.ShapeDtypeStruct((layers, rows, width), f32),) * 4 + (jax.ShapeDtypeStruct((SUB, width), f32),),
        in_specs=[vmem] * 5,
        out_specs=(vmem,) * 5,
        scratch_shapes=[
            pltpu.VMEM((2, rows + 4, layers + 2 * SUB, width), f32),
            pltpu.VMEM((2, layers, LANES), f32),
            pltpu.VMEM((2, layers, LANES), f32),
            pltpu.VMEM((2, layers, LANES), f32),
            pltpu.VMEM((2, rows_of_corners, 1, LANES), f32),
            pltpu.VMEM((2, rows_of_corners, 4, 1, LANES), f32),
            pltpu.VMEM((ITERS + 1, 2, layers, width), f32),
            pltpu.VMEM((ITERS + 2, rows, layers, width), f32),
            pltpu.VMEM((rows, layers, width), f32),
            pltpu.VMEM((rows, layers, width), f32),
            pltpu.VMEM((rows, layers, width), f32),
            pltpu.VMEM((2, rows, width), f32),
            pltpu.VMEM((2, rows, width), f32),
            pltpu.VMEM((2 * ITERS, SUB, LANES), f32),
            pltpu.VMEM((nx * ny, 1, LANES), f32),
            pltpu.VMEM((nx * ny, 1, LANES), f32),
            dma((2, chunks, 8)),
            dma((2, chunks, 8)),
            dma((2,)),
            dma((4, 2, chunks)),
            dma((nx * ny - 1,)),
            dma((nx * ny - 1,)),
            dma((nx * ny - 1,)),
            dma((nx * ny - 1,)),
            pltpu.VMEM((layers, rows, width), f32),
        ],
        compiler_params=pltpu.CompilerParams(
            collective_id=0, has_side_effects=True, vmem_limit_bytes=40 * 1024 * 1024
        ),
        name="krylov",
    )(forcing[0], wide_conduct, diag_add[0], active, friction)
    step = out_s[:1]
    solved, residual = out_x + step * out_p, out_r - step * out_q
    return tuple(o[None] for o in (solved, residual))


def solution(mesh):
    spec = P("group", None, "gx", "gy")
    flat = P("gx", "gy")
    return jax.shard_map(
        functools.partial(on_device, mesh.shape["gx"], mesh.shape["gy"]),
        mesh=mesh,
        in_specs=(spec, spec, spec, flat, flat),
        out_specs=(spec, spec),
        check_vma=False,
    )
```

```python
import functools

import jax
import jax.numpy as jnp
from jax import lax
from jax.experimental import pallas as pl
from jax.experimental.pallas import tpu as pltpu
from jax.sharding import PartitionSpec as P

ITERS = 6
far_weight = 0.25
cross_weight = 0.5
vertical_weight = 4.0
friction_gain = 8.0
SUB = 8
LANES = 128
CHUNK_TILES = (2, 1)


def coefficients(moments):
    def gram(j, k):
        return 0.5 * (moments[j + k] + moments[abs(j - k)])

    table = {
        (j, k): gram(j, k)
        for j in range(ITERS + 1)
        for k in range(j, ITERS + 1)
        if j + k < len(moments)
    }

    def form(a, b):
        terms = []
        for j in range(len(a)):
            row = None
            for k in range(len(b)):
                term = table[min(j, k), max(j, k)] * b[k]
                row = term if row is None else row + term
            terms.append(a[j] * row)
        return functools.reduce(lambda s, t: s + t, terms)

    def shift(e):
        out = [jnp.zeros_like(e[0]) for _ in range(len(e) + 1)]
        for k, value in enumerate(e):
            if k == 0:
                out[1] = out[1] + value
            else:
                out[k + 1] = out[k + 1] + 0.5 * value
                out[k - 1] = out[k - 1] + 0.5 * value
        return out

    left = [jnp.ones_like(moments[0])]
    direction = list(left)
    iterate = []
    norm_now = form(left, left)
    for iteration in range(ITERS):
        moved = shift(direction)
        applied = [
            (direction[k] - moved[k]) if k < len(direction) else -moved[k]
            for k in range(len(moved))
        ]
        if iteration + 1 == ITERS:
            table[iteration, ITERS] = 0.5 * moments[1]
            slope = 0.5 * direction[-1] * applied[-1]
            return iterate, left, direction, applied, norm_now, form(direction, applied), slope
        step = norm_now / form(direction, applied)
        iterate = [
            (iterate[k] if k < len(iterate) else 0.0) + step * direction[k]
            for k in range(len(direction))
        ]
        left = [
            (left[k] - step * applied[k]) if k < len(left) else -step * applied[k]
            for k in range(len(applied))
        ]
        norm_next = form(left, left)
        ratio = norm_next / norm_now
        direction = [
            left[k] + (ratio * direction[k] if k < len(direction) else 0.0)
            for k in range(len(left))
        ]
        norm_now = norm_next


def kernel(
    sizes,
    force,
    conduct,
    extra_half,
    active_cells,
    friction_cells,
    out_x,
    out_p,
    out_r,
    out_q,
    out_s,
    field,
    pack,
    rim_right,
    rim_left,
    corner,
    cornered,
    held,
    basis,
    coupling,
    scaled,
    diagonal,
    share,
    shared,
    partial,
    sum_early,
    sum_all,
    send_sem,
    recv_sem,
    share_sem,
    detour_sem,
    se_send,
    se_recv,
    sa_send,
    sa_recv,
    extra,
):
    nx, ny = sizes
    layers, rows, width = conduct.shape
    tiles = layers // SUB
    chunks = send_sem.shape[1]
    per = tiles // chunks
    deep = per * SUB
    group = 2 if 8 * deep <= LANES else 1
    gg, gx, gy = lax.axis_index("group"), lax.axis_index("gx"), lax.axis_index("gy")
    is_ice = gg == 0

    def there(dx, dy):
        ok = None
        for d, g, n in ((dx, gx, nx), (dy, gy, ny)):
            if d != 0:
                one = (g + d >= 0) & (g + d < n)
                ok = one if ok is None else ok & one
        return ok

    def at(dx, dy):
        return (gg, gx + dx, gy + dy)

    two = 2 * rows
    sides = ((-1, 0), (1, 0), (0, -1), (0, 1), (-1, -1), (1, -1), (-1, 1), (1, 1))

    def copy_of(i, p, c, span=2):
        dx, dy = sides[i]
        inner = pl.ds(pl.multiple_of(c * deep + SUB, SUB), deep)
        flat = pl.ds(pl.multiple_of(c * deep, SUB), deep)
        if i == 0:
            source = field.at[p, 2 : 2 + span, inner]
            target = field.at[p, rows + 2 : rows + 2 + span, inner]
        elif i == 1:
            source = field.at[p, rows : rows + span, inner]
            target = field.at[p, 0:span, inner]
        elif i == 2:
            source, target = pack.at[p, flat], rim_right.at[p, flat]
        elif i == 3:
            source, target = pack.at[p, flat], rim_left.at[p, flat]
        else:
            source, target = corner.at[p, c // group], cornered.at[p, c // group, i - 4]
        return pltpu.make_async_remote_copy(
            src_ref=source,
            dst_ref=target,
            send_sem=send_sem.at[p, c if i < 4 else c // group * group, i],
            recv_sem=recv_sem.at[p, c if i < 4 else c // group * group, i],
            device_id=at(dx, dy),
            device_id_type=pl.DeviceIdType.MESH,
        )

    detours = ((1, 3, 2, rows, 0), (2, 0, 1, 2, rows + 2)) if nx == 4 else ()
    relayed = gg == 1
    lag = min(3, chunks - 1)

    def each(toward, act, chosen=range(8)):
        for i in chosen:
            dx, dy = sides[i]
            ok = there(toward * dx, toward * dy)
            if i < 2 and detours:
                split = gx == ((2 - i) if toward > 0 else (1 + i))

                ok = ok & jnp.logical_not(split & relayed)

            @pl.when(ok)
            def _():
                act(i, 2)

    def away(path, p, c, slot):
        origin, relay, _, row, _ = path
        return pltpu.make_async_remote_copy(
            src_ref=field.at[p, row : row + 2, pl.ds(pl.multiple_of(c * deep + SUB, SUB), deep)],
            dst_ref=held.at[slot, :, pl.ds(pl.multiple_of(c * deep, SUB), deep)],
            send_sem=detour_sem.at[0, p, c],
            recv_sem=detour_sem.at[1, p, c],
            device_id=(gg, relay, gy),
            device_id_type=pl.DeviceIdType.MESH,
        )

    def onward(path, p, c, slot):
        _, _, end, _, row = path
        return pltpu.make_async_remote_copy(
            src_ref=held.at[slot, :, pl.ds(pl.multiple_of(c * deep, SUB), deep)],
            dst_ref=field.at[p, row : row + 2, pl.ds(pl.multiple_of(c * deep + SUB, SUB), deep)],
            send_sem=detour_sem.at[2, p, c],
            recv_sem=detour_sem.at[3, p, c],
            device_id=(gg, end, gy),
            device_id_type=pl.DeviceIdType.MESH,
        )

    def forward(message):
        slot = message // chunks
        c = message % chunks
        p = slot % 2
        for path in detours:
            @pl.when((gx == path[1]) & relayed)
            def _():
                @pl.when(slot >= 2)
                def _():
                    onward(path, p, c, slot).wait_send()

                away(path, p, c, slot).wait_recv()
                onward(path, p, c, slot).start()

    def first_of(c):
        return lax.rem(c, group) == 0

    def last_of(c):
        return (lax.rem(c, group) == group - 1) | (c == chunks - 1)

    def start_rows(p, c, slot):
        for path in detours:
            @pl.when((gx == path[0]) & relayed)
            def _():
                away(path, p, c, slot).start()
        for order in ((1, 0), (0, 1)):
            @pl.when((gx == 2) if order == (0, 1) else (gx != 2))
            def _():
                each(1, lambda i, span: copy_of(i, p, c, span).start(), order)

        @pl.when(last_of(c))
        def _():
            each(1, lambda i, span: copy_of(i, p, c, span).start(), range(4, 8))

    def start_rest(p, c):
        each(1, lambda i, span: copy_of(i, p, c, span).start(), range(2, 4))

    def start(p, c, slot):
        start_rows(p, c, slot)
        start_rest(p, c)

    def finish_rows(p, c):
        for path in detours:
            @pl.when((gx == path[2]) & relayed)
            def _():
                onward(path, p, c, 0).wait_recv()
        each(-1, lambda i, span: copy_of(i, p, c, span).wait_recv(), range(2))

        @pl.when(first_of(c))
        def _():
            each(-1, lambda i, span: copy_of(i, p, c, span).wait_recv(), range(4, 8))

    def finish_columns(p, c):
        each(-1, lambda i, span: copy_of(i, p, c, span).wait_recv(), range(2, 4))

    def finish_recv(p, c):
        finish_columns(p, c)
        finish_rows(p, c)

    def finish_send(p, c):
        for path in detours:
            @pl.when((gx == path[0]) & relayed)
            def _():
                away(path, p, c, 0).wait_send()
        each(1, lambda i, span: copy_of(i, p, c, span).wait_send(), range(4))

        @pl.when(first_of(c))
        def _():
            each(1, lambda i, span: copy_of(i, p, c, span).wait_send(), range(4, 8))

    barrier = pltpu.get_barrier_semaphore()

    def peers_all():
        me = gx * ny + gy
        out = []
        for o in range(1, nx * ny):
            peer = lax.rem(me + o, nx * ny)
            out.append((gg, peer // ny, lax.rem(peer, ny)))
        return out

    def greet(device):
        pl.semaphore_signal(
            barrier, inc=1, device_id=device, device_id_type=pl.DeviceIdType.MESH
        )

    greet((1 - gg, gx, gy))
    if max(nx, ny) < ITERS:
        met = jnp.int32(1)
        for dx, dy in sides:
            @pl.when(there(dx, dy))
            def _():
                greet(at(dx, dy))
            met = met + jnp.where(there(dx, dy), 1, 0).astype(jnp.int32)
        for origin, relay, end, _, _ in detours:
            for one, other in ((origin, relay), (relay, end)):
                for here, peer in ((one, other), (other, one)):
                    if abs(here - peer) > 1:
                        @pl.when(gx == here)
                        def _():
                            greet((gg, peer, gy))
                        met = met + jnp.where(gx == here, 1, 0).astype(jnp.int32)
    else:
        for device in peers_all():
            greet(device)
        met = jnp.int32(nx * ny)

    lane = lax.broadcasted_iota(jnp.int32, (SUB, LANES), 1)
    sub = lax.broadcasted_iota(jnp.int32, (SUB, width), 0)

    tile_row = lax.broadcasted_iota(jnp.int32, (SUB, LANES), 0)

    def spot(i, t):
        return lane == (i * per + t) * SUB + tile_row

    def pack_row(x, value, tile, t, corners):
        first, last = value[:, :LANES], value[:, width - LANES :]
        low = first if x == 0 else pltpu.roll(first, 2 * x, 1)
        high = pltpu.roll(last, (two + 2 * x - LANES + 2) % LANES, 1)
        tile = jnp.where((lane >= 2 * x) & (lane < 2 * x + 2), low, tile)
        tile = jnp.where((lane >= two + 2 * x) & (lane < two + 2 * x + 2), high, tile)
        for i, (at_x, y) in enumerate(
            ((0, 0), (rows - 1, 0), (0, width - 1), (rows - 1, width - 1))
        ):
            if x == at_x:
                column = jnp.broadcast_to(value[:, y : y + 1], (SUB, LANES))
                corners = jnp.where(spot(i, t), column, corners)
        return tile, corners

    def put_corner(p, c, corners):
        value = jnp.sum(corners, axis=0, keepdims=True)

        @pl.when(first_of(c))
        def _():
            corner[p, c // group] = value

        if group > 1:

            @pl.when(jnp.logical_not(first_of(c)))
            def _():
                corner[p, c // group] = corner[p, c // group] + pltpu.roll(value, LANES // 2, 1)

    active, friction = active_cells[...], friction_cells[...]

    def wide(array, x):
        return jnp.broadcast_to(array[x : x + 1, :], (SUB, width))

    blank = jnp.zeros((SUB, LANES), jnp.float32)
    zero = jnp.zeros((SUB, width), jnp.float32)

    def prepare(c):
        corners = blank
        for t in range(per):
            j = c * per + t
            ls = pl.ds(pl.multiple_of(j * SUB, SUB), SUB)
            tile = blank
            for x in range(rows):
                value = jnp.sqrt(conduct[ls, x, :]) * wide(active, x)
                coupling[x, ls, :] = value
                field[0, x + 2, pl.ds(pl.multiple_of(j * SUB + SUB, SUB), SUB), :] = value
                tile, corners = pack_row(x, value, tile, t, corners)
            pack[0, ls, :] = tile
        put_corner(0, c, corners)

    def first_pass(c, carry):
        start(0, c - 1, 0)

        @pl.when(c > lag)
        def _():
            forward(c - 1 - lag)

        prepare(c)
        return carry

    prepare(0)
    pl.semaphore_wait(barrier, met)
    lax.fori_loop(1, chunks, first_pass, 0)
    start(0, chunks - 1, 0)
    forward(chunks - 1 - lag)

    for p in range(2):
        for r, d in ((0, -1), (rows + 2, 1)):
            @pl.when(jnp.logical_not(there(d, 0)))
            def _():
                field[p, r : r + 2] = jnp.zeros((2, layers + 2 * SUB, width), jnp.float32)
        for r in range(2, rows + 2):
            for s in (0, SUB + layers):
                field[p, r, s : s + SUB] = jnp.zeros((SUB, width), jnp.float32)
        for ref, d in ((rim_left, -1), (rim_right, 1)):
            @pl.when(jnp.logical_not(there(0, d)))
            def _():
                ref[p] = jnp.zeros(ref.shape[1:], jnp.float32)
        for i in range(4):
            @pl.when(jnp.logical_not(there(-sides[4 + i][0], -sides[4 + i][1])))
            def _():
                for c in range(cornered.shape[1]):
                    cornered[p, c, i] = jnp.zeros((1, LANES), jnp.float32)

    def gather(j, total):
        for t in range(SUB):
            extra[j * SUB + t] = extra_half[j * SUB + t].astype(jnp.float32)
            total = total + force[j * SUB + t]
        return total

    total = lax.fori_loop(0, tiles, gather, jnp.zeros((rows, width), jnp.float32))
    share[0] = active * (total * (1.0 / layers))
    for x in range(rows):
        share[1, x : x + 1, :] = jnp.where(
            is_ice, coupling[x, 0:1, :], coupling[x, layers - 1 : layers, :]
        )

    to_partner = pltpu.make_async_remote_copy(
        src_ref=share,
        dst_ref=shared,
        send_sem=share_sem.at[0],
        recv_sem=share_sem.at[1],
        device_id=(1 - gg, gx, gy),
        device_id_type=pl.DeviceIdType.MESH,
    )
    to_partner.start()

    outer = tuple(x for x in range(rows) if x < 2 or x >= rows - 2)
    inner = tuple(x for x in range(rows) if x not in outer)

    def spread_block(p, c, t, xs):
        j = c * per + t
        here = pl.ds(pl.multiple_of(j * SUB + SUB, SUB), SUB)
        below = pl.ds(pl.multiple_of(j * SUB, SUB), SUB)
        above = pl.ds(pl.multiple_of(j * SUB + 2 * SUB, SUB), SUB)
        from_right, from_left = rim_right[p, below, :], rim_left[p, below, :]

        def column(i):
            row = jnp.broadcast_to(cornered[p, c // group, i], (SUB, LANES))
            if group > 1:
                row = jnp.where(first_of(c), row, pltpu.roll(row, LANES // 2, 1))
            return jnp.sum(jnp.where(spot(i, t), row, 0.0), axis=1, keepdims=True)

        def rim(x):
            right = from_right if x == 0 else pltpu.roll(from_right, LANES - 2 * x, 1)
            left = pltpu.roll(from_left, (LANES - 2 - two - 2 * x) % LANES, 1)
            return jnp.where(lane < LANES // 2, right, left)

        def line(x):
            if x == 0:
                edge = jnp.where(lane < LANES // 2, column(1), column(3))
            elif x == rows + 1:
                edge = jnp.where(lane < LANES // 2, column(0), column(2))
            else:
                edge = rim(x - 1)
            value = field[p, x + 1, here, :]
            return [value[:, l : l + LANES] for l in range(0, width, LANES)] + [edge]

        def shifted(tiles_in, by):
            count = len(tiles_in) - 1
            out = []
            for i in range(count):
                before, own, after = tiles_in[i - 1], tiles_in[i], tiles_in[i + 1]
                up = pltpu.roll(jnp.where(lane >= LANES - by, before, own), by, 1)
                down = pltpu.roll(jnp.where(lane < by, after, own), LANES - by, 1)
                out.append(up + down)
            return jnp.concatenate(out, axis=1)

        e = {}
        for x in xs:
            for i in range(x, x + 3):
                if i not in e:
                    e[i] = line(i)
            beside = [a + b for a, b in zip(e[x], e[x + 2])]
            h = [a + cross_weight * b for a, b in zip(e[x + 1], beside)]
            mine = field[p, x + 2, here, :]
            up = pltpu.roll(jnp.where(sub == 0, field[p, x + 2, above, :], mine), SUB - 1, 0)
            down = pltpu.roll(jnp.where(sub == SUB - 1, field[p, x + 2, below, :], mine), 1, 0)
            yield (
                shifted(h, 1)
                + jnp.concatenate(beside[:-1], axis=1)
                + far_weight
                * (shifted(e[x + 1], 2) + (field[p, x, here, :] + field[p, x + 4, here, :]))
                + vertical_weight * (up + down)
            )

    def fold(value):
        return functools.reduce(
            lambda s, t: s + t, [value[:, c : c + LANES] for c in range(0, width, LANES)]
        )

    to_partner.wait_recv()
    term = active * (shared[1] * shared[0])

    edge = jnp.where(is_ice, 0, layers - 1).astype(jnp.int32)

    def zeroth(c, acc):
        forward(chunks + c - lag)
        finish_recv(0, c)
        corners, packed = blank, [blank] * per
        for xs in (outer, inner):
            for t in range(per):
                j = c * per + t
                ls = pl.ds(pl.multiple_of(j * SUB, SUB), SUB)
                layer = sub + j * SUB
                at_edge = layer == edge
                at_bottom = layer == 0
                for x, around in zip(xs, list(spread_block(0, c, t, xs))):
                    own = coupling[x, ls, :]
                    diag = (
                        extra[ls, x, :]
                        + jnp.where(at_bottom, wide(friction, x), 0.0)
                        + own * around
                    )
                    inverse = 1.0 / diag
                    source = wide(active, x) * force[ls, x, :] + jnp.where(
                        at_edge, wide(term, x), 0.0
                    )
                    vector = inverse * source
                    diagonal[x, ls, :] = diag
                    scaled[x, ls, :] = inverse * own
                    basis[0, x, ls, :] = zero
                    basis[1, x, ls, :] = vector
                    value = own * vector
                    after = pl.ds(pl.multiple_of(j * SUB + SUB, SUB), SUB)
                    field[1, x + 2, after, :] = value
                    packed[t], corners = pack_row(x, value, packed[t], t, corners)
                    acc = acc + source * vector
                if xs is inner:
                    pack[1, ls, :] = packed[t]
            if xs is outer:
                put_corner(1, c, corners)
                start_rows(1, c, 1)
        start_rest(1, c)
        finish_send(0, c)
        return acc

    partial[0] = fold(lax.fori_loop(0, chunks, zeroth, zero))
    partial[1] = blank
    to_partner.wait_send()

    lane_row = lax.broadcasted_iota(jnp.int32, (1, LANES), 1)

    def copies(slots, me, devices, sends, recvs):
        return [
            pltpu.make_async_remote_copy(
                src_ref=slots.at[me],
                dst_ref=slots.at[me],
                send_sem=sends.at[o],
                recv_sem=recvs.at[o],
                device_id=device,
                device_id_type=pl.DeviceIdType.MESH,
            )
            for o, device in enumerate(devices)
        ]

    def row_of(slots):
        return functools.reduce(lambda s, t: s + t, [slots[o] for o in range(slots.shape[0])])

    def copies_early():
        return copies(sum_early, gx * ny + gy, peers_all(), se_send, se_recv)

    def early_start():
        row = jnp.zeros((1, LANES), jnp.float32)
        for m in range(2 * ITERS):
            value = jnp.sum(partial[m], axis=0, keepdims=True)
            value = jnp.sum(value, axis=1, keepdims=True)
            row = jnp.where(lane_row == m, jnp.broadcast_to(value, (1, LANES)), row)
        sum_early[gx * ny + gy] = row
        for copy in copies_early():
            copy.start()

    def early_finish():
        for copy in copies_early():
            copy.wait_recv()
        for copy in copies_early():
            copy.wait_send()

    def step(k, carry):
        p = lax.rem(k, 2)
        q = 1 - p
        gain = jnp.where(k == 1, 1.0, 2.0).astype(jnp.float32)

        def block(c, accs):
            own_acc, cross_acc = accs
            forward((k + 1) * chunks + c - lag)
            finish_recv(p, c)
            corners, packed = blank, [blank] * per
            for xs in (outer, inner):
                for t in range(per):
                    j = c * per + t
                    ls = pl.ds(pl.multiple_of(j * SUB, SUB), SUB)
                    vectors, values = [], []
                    for x, around in zip(xs, list(spread_block(p, c, t, xs))):
                        vector = gain * (scaled[x, ls, :] * around) - basis[k - 1, x, ls, :]
                        weighted = diagonal[x, ls, :] * vector
                        value = coupling[x, ls, :] * vector
                        own_acc = own_acc + weighted * vector
                        cross_acc = cross_acc + weighted * basis[k, x, ls, :]
                        packed[t], corners = pack_row(x, value, packed[t], t, corners)
                        vectors.append(vector)
                        values.append(value)
                    after = pl.ds(pl.multiple_of(j * SUB + SUB, SUB), SUB)
                    for x, vector, value in zip(xs, vectors, values):
                        basis[k + 1, x, ls, :] = vector
                        field[q, x + 2, after, :] = value
                    if xs is inner:
                        pack[q, ls, :] = packed[t]
                if xs is outer:
                    put_corner(q, c, corners)

                    start_rows(q, c, k + 1)

            start_rest(q, c)
            finish_send(p, c)
            return own_acc, cross_acc

        own_acc, cross_acc = lax.fori_loop(0, chunks, block, (zero, zero))
        partial[2 * k] = fold(own_acc)
        partial[2 * k + 1] = fold(cross_acc)

        return carry

    lax.fori_loop(1, ITERS, step, 0)
    early_start()
    now = ITERS % 2

    def final_rows(c, acc, xs):
        for t in range(per):
            ls = pl.ds(pl.multiple_of((c * per + t) * SUB, SUB), SUB)
            for x, around in zip(xs, list(spread_block(now, c, t, xs))):
                vector = 2.0 * (scaled[x, ls, :] * around) - basis[ITERS - 1, x, ls, :]
                acc = acc + diagonal[x, ls, :] * vector * basis[ITERS, x, ls, :]
                basis[ITERS + 1, x, ls, :] = vector
        return acc

    def final_block(c, acc):
        @pl.when(c < lag)
        def _():
            forward((ITERS + 1) * chunks + c - lag)

        finish_columns(now, c)
        acc = final_rows(c, acc, inner)
        finish_rows(now, c)
        return final_rows(c, acc, outer)

    acc = fold(lax.fori_loop(0, chunks, final_block, zero))
    sum_all[gx * ny + gy] = jnp.sum(acc, axis=0, keepdims=True)
    to_all = copies(sum_all, gx * ny + gy, peers_all(), sa_send, sa_recv)
    for copy in to_all:
        copy.start()

    def settle(c, carry):
        finish_send(now, c)
        for path in detours:
            @pl.when((gx == path[1]) & relayed)
            def _():
                for p in range(2):
                    onward(path, p, c, 0).wait_send()
        return carry

    lax.fori_loop(0, chunks, settle, 0)

    early_finish()
    total = row_of(sum_early)
    dots = [jnp.broadcast_to(total[:, m : m + 1], (SUB, LANES)) for m in range(2 * ITERS)]
    moments = [dots[0], dots[3]]
    for k in range(1, ITERS):
        if k > 1:
            moments.append(2.0 * dots[2 * k + 1] - moments[1])
        moments.append(2.0 * dots[2 * k] - moments[0])
    *lists, norm, fixed, slope = coefficients(moments)

    def widen(value):
        return jnp.concatenate([value] * (width // LANES), axis=1)

    iterate, left, direction, applied = [[widen(v) for v in values] for values in lists]

    def combined(values, us):
        return functools.reduce(lambda s, t: s + t, [a * u for a, u in zip(values, us)])

    def last(j, carry):
        ls = pl.ds(pl.multiple_of(j * SUB, SUB), SUB)
        for x in range(rows):
            us = [basis[k + 1, x, ls, :] for k in range(ITERS + 1)]
            diag = diagonal[x, ls, :]
            out_x[ls, x, :] = combined(iterate, us)
            out_p[ls, x, :] = combined(direction, us)
            out_r[ls, x, :] = diag * combined(left, us)
            out_q[ls, x, :] = diag * combined(applied, us)
        return carry

    lax.fori_loop(0, tiles, last, 0)

    for copy in to_all:
        copy.wait_recv()
    cross = jnp.sum(row_of(sum_all), axis=1, keepdims=True)
    cross = jnp.broadcast_to(cross, (SUB, LANES))
    out_s[...] = widen(norm / (fixed + slope * (2.0 * cross - moments[1])))
    for copy in to_all:
        copy.wait_send()


def on_device(nx, ny, forcing, conduct, diag_add, ice_mask, grounded):
    wide_conduct = conduct[0].astype(jnp.float32)
    wide_conduct, ice_mask, grounded = lax.optimization_barrier(
        (wide_conduct, ice_mask, grounded)
    )
    ice_cells, ground_cells = ice_mask.astype(jnp.float32), grounded.astype(jnp.float32)
    ocean = jnp.where(lax.axis_index("group") == 0, 0.0, 1.0)
    active = ice_cells * (1.0 - ocean * ground_cells)
    friction = (1.0 - ocean) * friction_gain * ground_cells * ice_cells
    _, layers, rows, width = forcing.shape
    tiles = layers // SUB
    chunks = tiles // next(t for t in CHUNK_TILES if tiles % t == 0)
    pairs = 2 if 8 * (layers // chunks) <= LANES else 1
    rows_of_corners = -(-chunks // pairs)
    f32 = jnp.float32
    block = jax.ShapeDtypeStruct((rows, layers, width), f32)
    vmem = pl.BlockSpec(memory_space=pltpu.VMEM)
    dma = pltpu.SemaphoreType.DMA
    out_x, out_p, out_r, out_q, out_s = pl.pallas_call(
        functools.partial(kernel, (nx, ny)),
        out_shape=(jax.ShapeDtypeStruct((layers, rows, width), f32),) * 4 + (jax.ShapeDtypeStruct((SUB, width), f32),),
        in_specs=[vmem] * 5,
        out_specs=(vmem,) * 5,
        scratch_shapes=[
            pltpu.VMEM((2, rows + 4, layers + 2 * SUB, width), f32),
            pltpu.VMEM((2, layers, LANES), f32),
            pltpu.VMEM((2, layers, LANES), f32),
            pltpu.VMEM((2, layers, LANES), f32),
            pltpu.VMEM((2, rows_of_corners, 1, LANES), f32),
            pltpu.VMEM((2, rows_of_corners, 4, 1, LANES), f32),
            pltpu.VMEM((ITERS + 1, 2, layers, width), f32),
            pltpu.VMEM((ITERS + 2, rows, layers, width), f32),
            pltpu.VMEM((rows, layers, width), f32),
            pltpu.VMEM((rows, layers, width), f32),
            pltpu.VMEM((rows, layers, width), f32),
            pltpu.VMEM((2, rows, width), f32),
            pltpu.VMEM((2, rows, width), f32),
            pltpu.VMEM((2 * ITERS, SUB, LANES), f32),
            pltpu.VMEM((nx * ny, 1, LANES), f32),
            pltpu.VMEM((nx * ny, 1, LANES), f32),
            dma((2, chunks, 8)),
            dma((2, chunks, 8)),
            dma((2,)),
            dma((4, 2, chunks)),
            dma((nx * ny - 1,)),
            dma((nx * ny - 1,)),
            dma((nx * ny - 1,)),
            dma((nx * ny - 1,)),
            pltpu.VMEM((layers, rows, width), f32),
        ],
        compiler_params=pltpu.CompilerParams(
            collective_id=0, has_side_effects=True, vmem_limit_bytes=40 * 1024 * 1024
        ),
        name="krylov",
    )(forcing[0], wide_conduct, diag_add[0], active, friction)
    step = out_s[:1]
    solved, residual = out_x + step * out_p, out_r - step * out_q
    return tuple(o[None] for o in (solved, residual))


def solution(mesh):
    spec = P("group", None, "gx", "gy")
    flat = P("gx", "gy")
    return jax.shard_map(
        functools.partial(on_device, mesh.shape["gx"], mesh.shape["gy"]),
        mesh=mesh,
        in_specs=(spec, spec, spec, flat, flat),
        out_specs=(spec, spec),
        check_vma=False,
    )
```

```python
import functools

import jax
import jax.numpy as jnp
from jax import lax
from jax.experimental import pallas as pl
from jax.experimental.pallas import tpu as pltpu
from jax.sharding import PartitionSpec as P

ITERS = 6
far_weight = 0.25
cross_weight = 0.5
vertical_weight = 4.0
friction_gain = 8.0
SUB = 8
LANES = 128
CHUNK_TILES = (2, 1)


def coefficients(moments):
    def gram(j, k):
        return 0.5 * (moments[j + k] + moments[abs(j - k)])

    table = {
        (j, k): gram(j, k)
        for j in range(ITERS + 1)
        for k in range(j, ITERS + 1)
        if j + k < len(moments)
    }

    def form(a, b):
        terms = []
        for j in range(len(a)):
            row = None
            for k in range(len(b)):
                term = table[min(j, k), max(j, k)] * b[k]
                row = term if row is None else row + term
            terms.append(a[j] * row)
        return functools.reduce(lambda s, t: s + t, terms)

    def shift(e):
        out = [jnp.zeros_like(e[0]) for _ in range(len(e) + 1)]
        for k, value in enumerate(e):
            if k == 0:
                out[1] = out[1] + value
            else:
                out[k + 1] = out[k + 1] + 0.5 * value
                out[k - 1] = out[k - 1] + 0.5 * value
        return out

    left = [jnp.ones_like(moments[0])]
    direction = list(left)
    iterate = []
    norm_now = form(left, left)
    for iteration in range(ITERS):
        moved = shift(direction)
        applied = [
            (direction[k] - moved[k]) if k < len(direction) else -moved[k]
            for k in range(len(moved))
        ]
        if iteration + 1 == ITERS:
            table[iteration, ITERS] = 0.5 * moments[1]
            slope = 0.5 * direction[-1] * applied[-1]
            return iterate, left, direction, applied, norm_now, form(direction, applied), slope
        step = norm_now / form(direction, applied)
        iterate = [
            (iterate[k] if k < len(iterate) else 0.0) + step * direction[k]
            for k in range(len(direction))
        ]
        left = [
            (left[k] - step * applied[k]) if k < len(left) else -step * applied[k]
            for k in range(len(applied))
        ]
        norm_next = form(left, left)
        ratio = norm_next / norm_now
        direction = [
            left[k] + (ratio * direction[k] if k < len(direction) else 0.0)
            for k in range(len(left))
        ]
        norm_now = norm_next


def kernel(
    sizes,
    force,
    conduct,
    extra_half,
    active_cells,
    friction_cells,
    out_x,
    out_p,
    out_r,
    out_q,
    out_s,
    field,
    pack,
    rim_right,
    rim_left,
    corner,
    cornered,
    held,
    basis,
    coupling,
    scaled,
    diagonal,
    share,
    shared,
    partial,
    sum_early,
    sum_all,
    send_sem,
    recv_sem,
    share_sem,
    detour_sem,
    se_send,
    se_recv,
    sa_send,
    sa_recv,
    extra,
):
    nx, ny = sizes
    layers, rows, width = conduct.shape
    tiles = layers // SUB
    chunks = send_sem.shape[1]
    per = tiles // chunks
    deep = per * SUB
    group = 2 if 8 * deep <= LANES else 1
    gg, gx, gy = lax.axis_index("group"), lax.axis_index("gx"), lax.axis_index("gy")
    is_ice = gg == 0

    def there(dx, dy):
        ok = None
        for d, g, n in ((dx, gx, nx), (dy, gy, ny)):
            if d != 0:
                one = (g + d >= 0) & (g + d < n)
                ok = one if ok is None else ok & one
        return ok

    def at(dx, dy):
        return (gg, gx + dx, gy + dy)

    two = 2 * rows
    sides = ((-1, 0), (1, 0), (0, -1), (0, 1), (-1, -1), (1, -1), (-1, 1), (1, 1))

    def copy_of(i, p, c, span=2):
        dx, dy = sides[i]
        inner = pl.ds(pl.multiple_of(c * deep + SUB, SUB), deep)
        flat = pl.ds(pl.multiple_of(c * deep, SUB), deep)
        if i == 0:
            source = field.at[p, 2 : 2 + span, inner]
            target = field.at[p, rows + 2 : rows + 2 + span, inner]
        elif i == 1:
            source = field.at[p, rows : rows + span, inner]
            target = field.at[p, 0:span, inner]
        elif i == 2:
            source, target = pack.at[p, flat], rim_right.at[p, flat]
        elif i == 3:
            source, target = pack.at[p, flat], rim_left.at[p, flat]
        else:
            source, target = corner.at[p, c // group], cornered.at[p, c // group, i - 4]
        return pltpu.make_async_remote_copy(
            src_ref=source,
            dst_ref=target,
            send_sem=send_sem.at[p, c if i < 4 else c // group * group, i],
            recv_sem=recv_sem.at[p, c if i < 4 else c // group * group, i],
            device_id=at(dx, dy),
            device_id_type=pl.DeviceIdType.MESH,
        )

    detours = ((1, 3, 2, rows, 0), (2, 0, 1, 2, rows + 2)) if nx == 4 else ()
    relayed = gg == 1
    lag = min(3, chunks - 1)

    def each(toward, act, chosen=range(8)):
        for i in chosen:
            dx, dy = sides[i]
            ok = there(toward * dx, toward * dy)
            if i < 2 and detours:
                split = gx == ((2 - i) if toward > 0 else (1 + i))

                ok = ok & jnp.logical_not(split & relayed)

            @pl.when(ok)
            def _():
                act(i, 2)

    def away(path, p, c, slot):
        origin, relay, _, row, _ = path
        return pltpu.make_async_remote_copy(
            src_ref=field.at[p, row : row + 2, pl.ds(pl.multiple_of(c * deep + SUB, SUB), deep)],
            dst_ref=held.at[slot, :, pl.ds(pl.multiple_of(c * deep, SUB), deep)],
            send_sem=detour_sem.at[0, p, c],
            recv_sem=detour_sem.at[1, p, c],
            device_id=(gg, relay, gy),
            device_id_type=pl.DeviceIdType.MESH,
        )

    def onward(path, p, c, slot):
        _, _, end, _, row = path
        return pltpu.make_async_remote_copy(
            src_ref=held.at[slot, :, pl.ds(pl.multiple_of(c * deep, SUB), deep)],
            dst_ref=field.at[p, row : row + 2, pl.ds(pl.multiple_of(c * deep + SUB, SUB), deep)],
            send_sem=detour_sem.at[2, p, c],
            recv_sem=detour_sem.at[3, p, c],
            device_id=(gg, end, gy),
            device_id_type=pl.DeviceIdType.MESH,
        )

    def forward(message):
        slot = message // chunks
        c = message % chunks
        p = slot % 2
        for path in detours:
            @pl.when((gx == path[1]) & relayed)
            def _():
                @pl.when(slot >= 2)
                def _():
                    onward(path, p, c, slot).wait_send()

                away(path, p, c, slot).wait_recv()
                onward(path, p, c, slot).start()

    def first_of(c):
        return lax.rem(c, group) == 0

    def last_of(c):
        return (lax.rem(c, group) == group - 1) | (c == chunks - 1)

    def start_rows(p, c, slot):
        for path in detours:
            @pl.when((gx == path[0]) & relayed)
            def _():
                away(path, p, c, slot).start()
        for order in ((1, 0), (0, 1)):
            @pl.when((gx == 2) if order == (0, 1) else (gx != 2))
            def _():
                each(1, lambda i, span: copy_of(i, p, c, span).start(), order)

        @pl.when(last_of(c))
        def _():
            each(1, lambda i, span: copy_of(i, p, c, span).start(), range(4, 8))

    def start_rest(p, c):
        each(1, lambda i, span: copy_of(i, p, c, span).start(), range(2, 4))

    def start(p, c, slot):
        start_rows(p, c, slot)
        start_rest(p, c)

    def finish_rows(p, c):
        for path in detours:
            @pl.when((gx == path[2]) & relayed)
            def _():
                onward(path, p, c, 0).wait_recv()
        each(-1, lambda i, span: copy_of(i, p, c, span).wait_recv(), range(2))

        @pl.when(first_of(c))
        def _():
            each(-1, lambda i, span: copy_of(i, p, c, span).wait_recv(), range(4, 8))

    def finish_columns(p, c):
        each(-1, lambda i, span: copy_of(i, p, c, span).wait_recv(), range(2, 4))

    def finish_recv(p, c):
        finish_columns(p, c)
        finish_rows(p, c)

    def finish_send(p, c):
        for path in detours:
            @pl.when((gx == path[0]) & relayed)
            def _():
                away(path, p, c, 0).wait_send()
        each(1, lambda i, span: copy_of(i, p, c, span).wait_send(), range(4))

        @pl.when(first_of(c))
        def _():
            each(1, lambda i, span: copy_of(i, p, c, span).wait_send(), range(4, 8))

    barrier = pltpu.get_barrier_semaphore()

    def peers_all():
        me = gx * ny + gy
        out = []
        middle = nx * ny // 2
        for o in sorted(range(1, nx * ny), key=lambda o: abs(o - middle)):
            peer = lax.rem(me + o, nx * ny)
            out.append((gg, peer // ny, lax.rem(peer, ny)))
        return out

    def greet(device):
        pl.semaphore_signal(
            barrier, inc=1, device_id=device, device_id_type=pl.DeviceIdType.MESH
        )

    greet((1 - gg, gx, gy))
    if max(nx, ny) < ITERS:
        met = jnp.int32(1)
        for dx, dy in sides:
            @pl.when(there(dx, dy))
            def _():
                greet(at(dx, dy))
            met = met + jnp.where(there(dx, dy), 1, 0).astype(jnp.int32)
        for origin, relay, end, _, _ in detours:
            for one, other in ((origin, relay), (relay, end)):
                for here, peer in ((one, other), (other, one)):
                    if abs(here - peer) > 1:
                        @pl.when(gx == here)
                        def _():
                            greet((gg, peer, gy))
                        met = met + jnp.where(gx == here, 1, 0).astype(jnp.int32)
    else:
        for device in peers_all():
            greet(device)
        met = jnp.int32(nx * ny)

    lane = lax.broadcasted_iota(jnp.int32, (SUB, LANES), 1)
    sub = lax.broadcasted_iota(jnp.int32, (SUB, width), 0)

    tile_row = lax.broadcasted_iota(jnp.int32, (SUB, LANES), 0)

    def spot(i, t):
        return lane == (i * per + t) * SUB + tile_row

    def pack_row(x, value, tile, t, corners):
        first, last = value[:, :LANES], value[:, width - LANES :]
        low = first if x == 0 else pltpu.roll(first, 2 * x, 1)
        high = pltpu.roll(last, (two + 2 * x - LANES + 2) % LANES, 1)
        tile = jnp.where((lane >= 2 * x) & (lane < 2 * x + 2), low, tile)
        tile = jnp.where((lane >= two + 2 * x) & (lane < two + 2 * x + 2), high, tile)
        for i, (at_x, y) in enumerate(
            ((0, 0), (rows - 1, 0), (0, width - 1), (rows - 1, width - 1))
        ):
            if x == at_x:
                column = jnp.broadcast_to(value[:, y : y + 1], (SUB, LANES))
                corners = jnp.where(spot(i, t), column, corners)
        return tile, corners

    def put_corner(p, c, corners):
        value = jnp.sum(corners, axis=0, keepdims=True)

        @pl.when(first_of(c))
        def _():
            corner[p, c // group] = value

        if group > 1:

            @pl.when(jnp.logical_not(first_of(c)))
            def _():
                corner[p, c // group] = corner[p, c // group] + pltpu.roll(value, LANES // 2, 1)

    active, friction = active_cells[...], friction_cells[...]

    def wide(array, x):
        return jnp.broadcast_to(array[x : x + 1, :], (SUB, width))

    blank = jnp.zeros((SUB, LANES), jnp.float32)
    zero = jnp.zeros((SUB, width), jnp.float32)

    def prepare(c):
        corners = blank
        for t in range(per):
            j = c * per + t
            ls = pl.ds(pl.multiple_of(j * SUB, SUB), SUB)
            tile = blank
            for x in range(rows):
                value = jnp.sqrt(conduct[ls, x, :]) * wide(active, x)
                coupling[x, ls, :] = value
                field[0, x + 2, pl.ds(pl.multiple_of(j * SUB + SUB, SUB), SUB), :] = value
                tile, corners = pack_row(x, value, tile, t, corners)
            pack[0, ls, :] = tile
        put_corner(0, c, corners)

    def first_pass(c, carry):
        start(0, c - 1, 0)

        @pl.when(c > lag)
        def _():
            forward(c - 1 - lag)

        prepare(c)
        return carry

    prepare(0)
    pl.semaphore_wait(barrier, met)
    lax.fori_loop(1, chunks, first_pass, 0)
    start(0, chunks - 1, 0)
    forward(chunks - 1 - lag)

    for p in range(2):
        for r, d in ((0, -1), (rows + 2, 1)):
            @pl.when(jnp.logical_not(there(d, 0)))
            def _():
                field[p, r : r + 2] = jnp.zeros((2, layers + 2 * SUB, width), jnp.float32)
        for r in range(2, rows + 2):
            for s in (0, SUB + layers):
                field[p, r, s : s + SUB] = jnp.zeros((SUB, width), jnp.float32)
        for ref, d in ((rim_left, -1), (rim_right, 1)):
            @pl.when(jnp.logical_not(there(0, d)))
            def _():
                ref[p] = jnp.zeros(ref.shape[1:], jnp.float32)
        for i in range(4):
            @pl.when(jnp.logical_not(there(-sides[4 + i][0], -sides[4 + i][1])))
            def _():
                for c in range(cornered.shape[1]):
                    cornered[p, c, i] = jnp.zeros((1, LANES), jnp.float32)

    def gather(j, total):
        for t in range(SUB):
            extra[j * SUB + t] = extra_half[j * SUB + t].astype(jnp.float32)
            total = total + force[j * SUB + t]
        return total

    total = lax.fori_loop(0, tiles, gather, jnp.zeros((rows, width), jnp.float32))
    share[0] = active * (total * (1.0 / layers))
    for x in range(rows):
        share[1, x : x + 1, :] = jnp.where(
            is_ice, coupling[x, 0:1, :], coupling[x, layers - 1 : layers, :]
        )

    to_partner = pltpu.make_async_remote_copy(
        src_ref=share,
        dst_ref=shared,
        send_sem=share_sem.at[0],
        recv_sem=share_sem.at[1],
        device_id=(1 - gg, gx, gy),
        device_id_type=pl.DeviceIdType.MESH,
    )
    to_partner.start()

    outer = tuple(x for x in range(rows) if x < 2 or x >= rows - 2)
    inner = tuple(x for x in range(rows) if x not in outer)

    def spread_block(p, c, t, xs):
        j = c * per + t
        here = pl.ds(pl.multiple_of(j * SUB + SUB, SUB), SUB)
        below = pl.ds(pl.multiple_of(j * SUB, SUB), SUB)
        above = pl.ds(pl.multiple_of(j * SUB + 2 * SUB, SUB), SUB)
        from_right, from_left = rim_right[p, below, :], rim_left[p, below, :]

        def column(i):
            row = jnp.broadcast_to(cornered[p, c // group, i], (SUB, LANES))
            if group > 1:
                row = jnp.where(first_of(c), row, pltpu.roll(row, LANES // 2, 1))
            return jnp.sum(jnp.where(spot(i, t), row, 0.0), axis=1, keepdims=True)

        def rim(x):
            right = from_right if x == 0 else pltpu.roll(from_right, LANES - 2 * x, 1)
            left = pltpu.roll(from_left, (LANES - 2 - two - 2 * x) % LANES, 1)
            return jnp.where(lane < LANES // 2, right, left)

        def line(x):
            if x == 0:
                edge = jnp.where(lane < LANES // 2, column(1), column(3))
            elif x == rows + 1:
                edge = jnp.where(lane < LANES // 2, column(0), column(2))
            else:
                edge = rim(x - 1)
            value = field[p, x + 1, here, :]
            return [value[:, l : l + LANES] for l in range(0, width, LANES)] + [edge]

        def shifted(tiles_in, by):
            count = len(tiles_in) - 1
            out = []
            for i in range(count):
                before, own, after = tiles_in[i - 1], tiles_in[i], tiles_in[i + 1]
                up = pltpu.roll(jnp.where(lane >= LANES - by, before, own), by, 1)
                down = pltpu.roll(jnp.where(lane < by, after, own), LANES - by, 1)
                out.append(up + down)
            return jnp.concatenate(out, axis=1)

        e = {}
        for x in xs:
            for i in range(x, x + 3):
                if i not in e:
                    e[i] = line(i)
            beside = [a + b for a, b in zip(e[x], e[x + 2])]
            h = [a + cross_weight * b for a, b in zip(e[x + 1], beside)]
            mine = field[p, x + 2, here, :]
            up = pltpu.roll(jnp.where(sub == 0, field[p, x + 2, above, :], mine), SUB - 1, 0)
            down = pltpu.roll(jnp.where(sub == SUB - 1, field[p, x + 2, below, :], mine), 1, 0)
            yield (
                shifted(h, 1)
                + jnp.concatenate(beside[:-1], axis=1)
                + far_weight
                * (shifted(e[x + 1], 2) + (field[p, x, here, :] + field[p, x + 4, here, :]))
                + vertical_weight * (up + down)
            )

    def fold(value):
        return functools.reduce(
            lambda s, t: s + t, [value[:, c : c + LANES] for c in range(0, width, LANES)]
        )

    to_partner.wait_recv()
    term = active * (shared[1] * shared[0])

    edge = jnp.where(is_ice, 0, layers - 1).astype(jnp.int32)

    def zeroth(c, acc):
        forward(chunks + c - lag)
        finish_recv(0, c)
        corners, packed = blank, [blank] * per
        for xs in (outer, inner):
            for t in range(per):
                j = c * per + t
                ls = pl.ds(pl.multiple_of(j * SUB, SUB), SUB)
                layer = sub + j * SUB
                at_edge = layer == edge
                at_bottom = layer == 0
                for x, around in zip(xs, list(spread_block(0, c, t, xs))):
                    own = coupling[x, ls, :]
                    diag = (
                        extra[ls, x, :]
                        + jnp.where(at_bottom, wide(friction, x), 0.0)
                        + own * around
                    )
                    inverse = 1.0 / diag
                    source = wide(active, x) * force[ls, x, :] + jnp.where(
                        at_edge, wide(term, x), 0.0
                    )
                    vector = inverse * source
                    diagonal[x, ls, :] = diag
                    scaled[x, ls, :] = inverse * own
                    basis[0, x, ls, :] = zero
                    basis[1, x, ls, :] = vector
                    value = own * vector
                    after = pl.ds(pl.multiple_of(j * SUB + SUB, SUB), SUB)
                    field[1, x + 2, after, :] = value
                    packed[t], corners = pack_row(x, value, packed[t], t, corners)
                    acc = acc + source * vector
                if xs is inner:
                    pack[1, ls, :] = packed[t]
            if xs is outer:
                put_corner(1, c, corners)
                start_rows(1, c, 1)
        start_rest(1, c)
        finish_send(0, c)
        return acc

    partial[0] = fold(lax.fori_loop(0, chunks, zeroth, zero))
    partial[1] = blank
    to_partner.wait_send()

    lane_row = lax.broadcasted_iota(jnp.int32, (1, LANES), 1)

    def copies(slots, me, devices, sends, recvs):
        return [
            pltpu.make_async_remote_copy(
                src_ref=slots.at[me],
                dst_ref=slots.at[me],
                send_sem=sends.at[o],
                recv_sem=recvs.at[o],
                device_id=device,
                device_id_type=pl.DeviceIdType.MESH,
            )
            for o, device in enumerate(devices)
        ]

    def row_of(slots):
        terms = [slots[o] for o in range(slots.shape[0])]
        while len(terms) > 1:
            pairs = [a + b for a, b in zip(terms[::2], terms[1::2])]
            terms = pairs + terms[len(pairs) * 2 :]
        return terms[0]

    def copies_early():
        return copies(sum_early, gx * ny + gy, peers_all(), se_send, se_recv)

    def early_start():
        row = jnp.zeros((1, LANES), jnp.float32)
        for m in range(2 * ITERS):
            value = jnp.sum(partial[m], axis=0, keepdims=True)
            value = jnp.sum(value, axis=1, keepdims=True)
            row = jnp.where(lane_row == m, jnp.broadcast_to(value, (1, LANES)), row)
        sum_early[gx * ny + gy] = row
        for copy in copies_early():
            copy.start()

    def early_finish():
        for copy in copies_early():
            copy.wait_recv()
        for copy in copies_early():
            copy.wait_send()

    def step(k, carry):
        p = lax.rem(k, 2)
        q = 1 - p
        gain = jnp.where(k == 1, 1.0, 2.0).astype(jnp.float32)

        def block(c, accs):
            own_acc, cross_acc = accs
            forward((k + 1) * chunks + c - lag)
            finish_recv(p, c)
            corners, packed = blank, [blank] * per
            for xs in (outer, inner):
                for t in range(per):
                    j = c * per + t
                    ls = pl.ds(pl.multiple_of(j * SUB, SUB), SUB)
                    vectors, values = [], []
                    for x, around in zip(xs, list(spread_block(p, c, t, xs))):
                        vector = gain * (scaled[x, ls, :] * around) - basis[k - 1, x, ls, :]
                        weighted = diagonal[x, ls, :] * vector
                        value = coupling[x, ls, :] * vector
                        own_acc = own_acc + weighted * vector
                        cross_acc = cross_acc + weighted * basis[k, x, ls, :]
                        packed[t], corners = pack_row(x, value, packed[t], t, corners)
                        vectors.append(vector)
                        values.append(value)
                    after = pl.ds(pl.multiple_of(j * SUB + SUB, SUB), SUB)
                    for x, vector, value in zip(xs, vectors, values):
                        basis[k + 1, x, ls, :] = vector
                        field[q, x + 2, after, :] = value
                    if xs is inner:
                        pack[q, ls, :] = packed[t]
                if xs is outer:
                    put_corner(q, c, corners)

                    start_rows(q, c, k + 1)

            start_rest(q, c)
            finish_send(p, c)
            return own_acc, cross_acc

        own_acc, cross_acc = lax.fori_loop(0, chunks, block, (zero, zero))
        partial[2 * k] = fold(own_acc)
        partial[2 * k + 1] = fold(cross_acc)

        return carry

    lax.fori_loop(1, ITERS, step, 0)
    early_start()
    now = ITERS % 2

    def final_rows(c, acc, xs):
        for t in range(per):
            ls = pl.ds(pl.multiple_of((c * per + t) * SUB, SUB), SUB)
            for x, around in zip(xs, list(spread_block(now, c, t, xs))):
                vector = 2.0 * (scaled[x, ls, :] * around) - basis[ITERS - 1, x, ls, :]
                acc = acc + diagonal[x, ls, :] * vector * basis[ITERS, x, ls, :]
                basis[ITERS + 1, x, ls, :] = vector
        return acc

    def final_block(c, acc):
        @pl.when(c < lag)
        def _():
            forward((ITERS + 1) * chunks + c - lag)

        finish_columns(now, c)
        acc = final_rows(c, acc, inner)
        finish_rows(now, c)
        return final_rows(c, acc, outer)

    acc = fold(lax.fori_loop(0, chunks, final_block, zero))
    sum_all[gx * ny + gy] = jnp.sum(acc, axis=0, keepdims=True)
    to_all = copies(sum_all, gx * ny + gy, peers_all(), sa_send, sa_recv)
    for copy in to_all:
        copy.start()

    def settle(c, carry):
        finish_send(now, c)
        for path in detours:
            @pl.when((gx == path[1]) & relayed)
            def _():
                for p in range(2):
                    onward(path, p, c, 0).wait_send()
        return carry

    lax.fori_loop(0, chunks, settle, 0)

    early_finish()
    total = row_of(sum_early)
    dots = [jnp.broadcast_to(total[:, m : m + 1], (SUB, LANES)) for m in range(2 * ITERS)]
    moments = [dots[0], dots[3]]
    for k in range(1, ITERS):
        if k > 1:
            moments.append(2.0 * dots[2 * k + 1] - moments[1])
        moments.append(2.0 * dots[2 * k] - moments[0])
    *lists, norm, fixed, slope = coefficients(moments)

    def widen(value):
        return jnp.concatenate([value] * (width // LANES), axis=1)

    iterate, left, direction, applied = [[widen(v) for v in values] for values in lists]

    def combined(values, us):
        return functools.reduce(lambda s, t: s + t, [a * u for a, u in zip(values, us)])

    def last(j, carry):
        ls = pl.ds(pl.multiple_of(j * SUB, SUB), SUB)
        for x in range(rows):
            us = [basis[k + 1, x, ls, :] for k in range(ITERS + 1)]
            diag = diagonal[x, ls, :]
            out_x[ls, x, :] = combined(iterate, us)
            out_p[ls, x, :] = combined(direction, us)
            out_r[ls, x, :] = diag * combined(left, us)
            out_q[ls, x, :] = diag * combined(applied, us)
        return carry

    lax.fori_loop(0, tiles, last, 0)

    for copy in to_all:
        copy.wait_send()
    for copy in to_all:
        copy.wait_recv()
    cross = jnp.sum(row_of(sum_all), axis=1, keepdims=True)
    cross = jnp.broadcast_to(cross, (SUB, LANES))
    out_s[...] = widen(norm / (fixed + slope * (2.0 * cross - moments[1])))


def on_device(nx, ny, forcing, conduct, diag_add, ice_mask, grounded):
    wide_conduct = conduct[0].astype(jnp.float32)
    wide_conduct, ice_mask, grounded = lax.optimization_barrier(
        (wide_conduct, ice_mask, grounded)
    )
    ice_cells, ground_cells = ice_mask.astype(jnp.float32), grounded.astype(jnp.float32)
    ocean = jnp.where(lax.axis_index("group") == 0, 0.0, 1.0)
    active = ice_cells * (1.0 - ocean * ground_cells)
    friction = (1.0 - ocean) * friction_gain * ground_cells * ice_cells
    _, layers, rows, width = forcing.shape
    tiles = layers // SUB
    chunks = tiles // next(t for t in CHUNK_TILES if tiles % t == 0)
    pairs = 2 if 8 * (layers // chunks) <= LANES else 1
    rows_of_corners = -(-chunks // pairs)
    f32 = jnp.float32
    block = jax.ShapeDtypeStruct((rows, layers, width), f32)
    vmem = pl.BlockSpec(memory_space=pltpu.VMEM)
    dma = pltpu.SemaphoreType.DMA
    out_x, out_p, out_r, out_q, out_s = pl.pallas_call(
        functools.partial(kernel, (nx, ny)),
        out_shape=(jax.ShapeDtypeStruct((layers, rows, width), f32),) * 4 + (jax.ShapeDtypeStruct((SUB, width), f32),),
        in_specs=[vmem] * 5,
        out_specs=(vmem,) * 5,
        scratch_shapes=[
            pltpu.VMEM((2, rows + 4, layers + 2 * SUB, width), f32),
            pltpu.VMEM((2, layers, LANES), f32),
            pltpu.VMEM((2, layers, LANES), f32),
            pltpu.VMEM((2, layers, LANES), f32),
            pltpu.VMEM((2, rows_of_corners, 1, LANES), f32),
            pltpu.VMEM((2, rows_of_corners, 4, 1, LANES), f32),
            pltpu.VMEM((ITERS + 1, 2, layers, width), f32),
            pltpu.VMEM((ITERS + 2, rows, layers, width), f32),
            pltpu.VMEM((rows, layers, width), f32),
            pltpu.VMEM((rows, layers, width), f32),
            pltpu.VMEM((rows, layers, width), f32),
            pltpu.VMEM((2, rows, width), f32),
            pltpu.VMEM((2, rows, width), f32),
            pltpu.VMEM((2 * ITERS, SUB, LANES), f32),
            pltpu.VMEM((nx * ny, 1, LANES), f32),
            pltpu.VMEM((nx * ny, 1, LANES), f32),
            dma((2, chunks, 8)),
            dma((2, chunks, 8)),
            dma((2,)),
            dma((4, 2, chunks)),
            dma((nx * ny - 1,)),
            dma((nx * ny - 1,)),
            dma((nx * ny - 1,)),
            dma((nx * ny - 1,)),
            pltpu.VMEM((layers, rows, width), f32),
        ],
        compiler_params=pltpu.CompilerParams(
            collective_id=0, has_side_effects=True, vmem_limit_bytes=40 * 1024 * 1024
        ),
        name="krylov",
    )(forcing[0], wide_conduct, diag_add[0], active, friction)
    step = out_s[:1]
    solved, residual = out_x + step * out_p, out_r - step * out_q
    return tuple(o[None] for o in (solved, residual))


def solution(mesh):
    spec = P("group", None, "gx", "gy")
    flat = P("gx", "gy")
    return jax.shard_map(
        functools.partial(on_device, mesh.shape["gx"], mesh.shape["gy"]),
        mesh=mesh,
        in_specs=(spec, spec, spec, flat, flat),
        out_specs=(spec, spec),
        check_vma=False,
    )
```
